128 devices in a mesh: rep: 1, dp: 128 (over x, y, z, core).
Axes of the slice: x: 4, y: 4, z: 4, core: 2. Of those that a mesh axis runs over, the one named last changes fastest.
Arguments:
- x: bfloat16 [128, 1024, 1280], P(('rep', 'dp'))
- dy: bfloat16 [128, 1024, 1280], P(('rep', 'dp'))
- wq: bfloat16 [1, 1280, 3072], replicated
- wk: bfloat16 [1, 1280, 256], replicated
- wv: bfloat16 [1, 1280, 256], replicated
- wo: bfloat16 [1, 3072, 1280], replicated
- w_gate: bfloat16 [1, 1280, 3072], replicated
- w_up: bfloat16 [1, 1280, 3072], replicated
- w_down: bfloat16 [1, 3072, 1280], replicated
- m_wq: float32 [1, 1280, 3072], P(None, 'dp')
- m_wk: float32 [1, 1280, 256], P(None, 'dp')
- m_wv: float32 [1, 1280, 256], P(None, 'dp')
- m_wo: float32 [1, 3072, 1280], P(None, 'dp')
- m_w_gate: float32 [1, 1280, 3072], P(None, 'dp')
- m_w_up: float32 [1, 1280, 3072], P(None, 'dp')
- m_w_down: float32 [1, 3072, 1280], P(None, 'dp')
- v_wq: float32 [1, 1280, 3072], P(None, 'dp')
- v_wk: float32 [1, 1280, 256], P(None, 'dp')
- v_wv: float32 [1, 1280, 256], P(None, 'dp')
- v_wo: float32 [1, 3072, 1280], P(None, 'dp')
- v_w_gate: float32 [1, 1280, 3072], P(None, 'dp')
- v_w_up: float32 [1, 1280, 3072], P(None, 'dp')
- v_w_down: float32 [1, 3072, 1280], P(None, 'dp')
Outputs:
- output 1: bfloat16 [1, 1280, 3072], P('rep')
- output 2: bfloat16 [1, 1280, 256], P('rep')
- output 3: bfloat16 [1, 1280, 256], P('rep')
- output 4: bfloat16 [1, 3072, 1280], P('rep')
- output 5: bfloat16 [1, 1280, 3072], P('rep')
- output 6: bfloat16 [1, 1280, 3072], P('rep')
- output 7: bfloat16 [1, 3072, 1280], P('rep')
- output 8: float32 [1, 1280, 3072], P('rep', 'dp')
- output 9: float32 [1, 1280, 256], P('rep', 'dp')
- output 10: float32 [1, 1280, 256], P('rep', 'dp')
- output 11: float32 [1, 3072, 1280], P('rep', 'dp')
- output 12: float32 [1, 1280, 3072], P('rep', 'dp')
- output 13: float32 [1, 1280, 3072], P('rep', 'dp')
- output 14: float32 [1, 3072, 1280], P('rep', 'dp')
- output 15: float32 [1, 1280, 3072], P('rep', 'dp')
- output 16: float32 [1, 1280, 256], P('rep', 'dp')
- output 17: float32 [1, 1280, 256], P('rep', 'dp')
- output 18: float32 [1, 3072, 1280], P('rep', 'dp')
- output 19: float32 [1, 1280, 3072], P('rep', 'dp')
- output 20: float32 [1, 1280, 3072], P('rep', 'dp')
- output 21: float32 [1, 3072, 1280], P('rep', 'dp')
All inputs are finite; a program needn't handle non-finite values.
Results may differ from the reference program's by a relative error of at most 0.024.
Values are sent between devices in bfloat16 or wider.
A program may use at most 1.5 GiB of HBM per device.

```python
import jax
import jax.numpy as jnp
from jax import lax

SEQUENCES = 128
TOKENS = 1024
D = 1280
HEADS = 24
KV_HEADS = 2
HEAD = 128
FF = 3072
LAYERS = 1
THETA = 10000
NAMES = ("wq", "wk", "wv", "wo", "w_gate", "w_up", "w_down")
SHAPES = {
    "wq": (LAYERS, D, HEADS * HEAD),
    "wk": (LAYERS, D, KV_HEADS * HEAD),
    "wv": (LAYERS, D, KV_HEADS * HEAD),
    "wo": (LAYERS, HEADS * HEAD, D),
    "w_gate": (LAYERS, D, FF),
    "w_up": (LAYERS, D, FF),
    "w_down": (LAYERS, FF, D),
}


def bump(key, n, height):
    away = (jnp.arange(n, dtype=jnp.int32) - jax.random.randint(key, (), 0, n, jnp.int32)) % n
    return jnp.where(away < n // 8, height, 1.0)


def together(key, own, strength):
    shared = jax.random.normal(key, own.shape[1:], jnp.float32)
    return (own + strength * shared) * lax.rsqrt(1 + strength * strength)


def setup_inputs(seed: int = 0, part: int = 0) -> dict:
    kx, kdy, ka, kb, kz, kf, kh, kl, *keys = jax.random.split(jax.random.key(seed), 8 + 3 * len(NAMES))
    kx, kdy, ka, kb = (jax.random.fold_in(k, part) for k in (kx, kdy, ka, kb))
    kw, km, kv = (keys[i::3] for i in range(3))
    shape = (SEQUENCES, TOKENS, D)
    much_x, much_dy = jax.random.uniform(kz, (2,), jnp.float32, 0.0, 1.0)
    loud = 2.0 ** jax.random.uniform(jax.random.fold_in(kz, 1), (), jnp.float32, -1.0, 2.0)
    layers = 2.0 ** jax.random.uniform(kl, (LAYERS, 1, 1), jnp.float32, -1.0, 1.0)
    times = {"wq": 1.0, "wk": 1.0, "wv": 2.0, "wo": layers, "w_gate": 1.0, "w_up": bump(kh, FF, 4.0), "w_down": layers}
    x = together(ka, jax.random.normal(kx, shape, jnp.float32), much_x) * bump(kf, D, 4.0)
    dy = together(kb, jax.random.normal(kdy, shape, jnp.float32), much_dy)
    drawn = {"x": x.astype(jnp.bfloat16), "dy": (loud * dy * (SEQUENCES * TOKENS) ** -0.5).astype(jnp.bfloat16)}
    for key, name in zip(kw, NAMES, strict=True):
        drawn[name] = (jax.random.normal(key, SHAPES[name], jnp.float32) * SHAPES[name][1] ** -0.5 * times[name]).astype(jnp.bfloat16)
    for key, name in zip(km, NAMES, strict=True):
        drawn[f"m_{name}"] = 0.1 * jax.random.normal(key, SHAPES[name], jnp.float32)
    for key, name in zip(kv, NAMES, strict=True):
        drawn[f"v_{name}"] = loud * loud * jax.random.uniform(key, SHAPES[name], jnp.float32, 0.2, 0.6)
    return drawn


def matmul(a, w):
    return jnp.dot(a, w, preferred_element_type=jnp.float32).astype(jnp.bfloat16)


def normed(h):
    wide = h.astype(jnp.float32)
    scale = lax.rsqrt(jnp.mean(wide**2, -1, keepdims=True) + 1e-6)
    return (wide * scale).astype(jnp.bfloat16)


def turned(t, theta):
    half = t.shape[-1] // 2
    angle = jnp.arange(t.shape[0], dtype=jnp.float32)[:, None] * theta ** (-jnp.arange(half, dtype=jnp.float32) / half)
    cos, sin = jnp.cos(angle)[:, None], jnp.sin(angle)[:, None]
    a, b = t[..., :half].astype(jnp.float32), t[..., half:].astype(jnp.float32)
    return jnp.concatenate([a * cos - b * sin, b * cos + a * sin], -1).astype(jnp.bfloat16)


def seen_by(q, k, v):
    tokens, kv = q.shape[0], k.shape[1]
    q = q.reshape(tokens, kv, -1, q.shape[-1])
    scores = jnp.einsum("tgsd,ugd->gstu", q.astype(jnp.float32), k.astype(jnp.float32)) * q.shape[-1] ** -0.5
    place = jnp.arange(tokens)
    weights = jax.nn.softmax(jnp.where(place[:, None] >= place, scores, -jnp.inf), -1).astype(jnp.bfloat16)
    return jnp.einsum("gstu,ugd->tgsd", weights.astype(jnp.float32), v.astype(jnp.float32)).astype(jnp.bfloat16).reshape(tokens, -1)


def layer(h, w):
    a = normed(h)
    q, k = (turned(matmul(a, w[name]).reshape(h.shape[0], -1, HEAD), THETA) for name in ("wq", "wk"))
    h = h + matmul(seen_by(q, k, matmul(a, w["wv"]).reshape(h.shape[0], -1, HEAD)), w["wo"])
    b = normed(h)
    gate = jnp.dot(b, w["w_gate"], preferred_element_type=jnp.float32)
    up = jnp.dot(b, w["w_up"], preferred_element_type=jnp.float32)
    return h + matmul((jax.nn.silu(gate) * up).astype(jnp.bfloat16), w["w_down"])


def adamw(w, m, v, g):
    m = 0.9 * m + 0.1 * g
    v = 0.95 * v + 0.05 * g * g
    step = m * lax.rsqrt(v + 1e-8) + 0.1 * w
    return (w - 0.02 * step).astype(jnp.bfloat16), m, v


def stack(weights, h):
    return lax.scan(lambda h, w: (layer(h, w), None), h, weights)[0]


def reference(x, dy, wq, wk, wv, wo, w_gate, w_up, w_down, m_wq, m_wk, m_wv, m_wo, m_w_gate, m_w_up, m_w_down, v_wq, v_wk, v_wv, v_wo, v_w_gate, v_w_up, v_w_down):
    weights = dict(zip(NAMES, (wq, wk, wv, wo, w_gate, w_up, w_down), strict=True))

    def take(so_far, sequence):
        h, by_y = sequence
        _, back = jax.vjp(stack, weights, h)
        by_weights, by_h = back(by_y)
        return jax.tree.map(lambda total, term: total + term.astype(jnp.float32), so_far, by_weights), by_h

    none_yet = {name: jnp.zeros(w.shape, jnp.float32) for name, w in weights.items()}
    by_weights, by_x = lax.scan(take, none_yet, (x, dy))
    gradients = [by_weights[name].astype(jnp.bfloat16).astype(jnp.float32) for name in NAMES]
    first = (m_wq, m_wk, m_wv, m_wo, m_w_gate, m_w_up, m_w_down)
    second = (v_wq, v_wk, v_wv, v_wo, v_w_gate, v_w_up, v_w_down)
    new = [adamw(weights[name].astype(jnp.float32), m, v, g) for name, m, v, g in zip(NAMES, first, second, gradients, strict=True)]
    return tuple(one[which] for which in range(3) for one in new)
```

```python
import functools

import jax
import jax.numpy as jnp
from jax import lax
from jax.experimental import pallas as pl
from jax.experimental.pallas import tpu as pltpu
from jax.sharding import PartitionSpec as P

NEG = -1e30
HIDDEN = 2 * NEG
LOG2E = 1.4426950408889634
HEAD = 128
THETA = 10000
SPAN = 12 * HEAD
SCALE = HEAD**-0.5
STRIP = 512
KEYS = 256
NAMES = ("wq", "wk", "wv", "wo", "w_gate", "w_up", "w_down")
MIB = 2**20
F32, BF16 = jnp.float32, jnp.bfloat16


def _dot(a, b, ca, cb):
    return lax.dot_general(a, b, (((ca,), (cb,)), ((), ())), preferred_element_type=F32)


def angles(tokens):
    half = HEAD // 2
    angle = jnp.arange(tokens, dtype=F32)[:, None] * THETA ** (-jnp.arange(half, dtype=F32) / half)
    cos, sin = jnp.cos(angle), jnp.sin(angle)
    return jnp.concatenate([cos, cos], 1), jnp.concatenate([-sin, sin], 1)


def swapped(t):
    return pltpu.roll(t, HEAD // 2, 1)


def turn(t, cos, sin):
    t = t.astype(F32)
    return (t * cos + swapped(t) * sin).astype(BF16)


def turn_back(t, cos, sin):
    t = t.astype(BF16).astype(F32)
    return (t * cos + swapped(t * sin)).astype(BF16)


def lanes(n):
    return slice(n * HEAD, (n + 1) * HEAD)


def strips(bq):
    per = STRIP // bq
    return [range(n, n + per) for n in range(0, SPAN // HEAD, per)]


def stacked(ref, heads):
    return jnp.concatenate([ref[:, lanes(n)] for n in heads], axis=0)


def row(ref, heads):
    return jnp.concatenate([ref[n : n + 1, :] for n in heads], axis=1)


def gaps(bq):
    shape = (KEYS, STRIP)
    return lax.rem(lax.broadcasted_iota(jnp.int32, shape, 1), bq) - lax.broadcasted_iota(jnp.int32, shape, 0)


def forward(q_ref, k_ref, v_ref, cos_ref, sin_ref, out_ref, lse_ref, qt_ref, kt_ref, top_s, mix_s):
    bq = q_ref.shape[0]
    iq = pl.program_id(1)
    e = SCALE * LOG2E

    @pl.when(iq == 0)
    def _():
        kt_ref[...] = turn(k_ref[...], cos_ref[...], sin_ref[...])

    here = pl.ds(pl.multiple_of(iq * bq, bq), bq)
    cos, sin = cos_ref[here, :], sin_ref[here, :]
    for n in range(SPAN // HEAD):
        qt_ref[:, lanes(n)] = turn(q_ref[:, lanes(n)], cos, sin)
    top_s[...] = jnp.full_like(top_s, NEG)
    mix_s[...] = jnp.zeros_like(mix_s)
    ones = jnp.ones((8, KEYS), BF16)
    pieces = strips(bq)

    def block(j, masked):
        keys = pl.ds(pl.multiple_of(j * KEYS, KEYS), KEYS)
        values = jnp.concatenate([v_ref[keys, :].T, ones], axis=0)
        scores = [_dot(kt_ref[keys, :], stacked(qt_ref, heads), 1, 1) for heads in pieces]
        weights, keeps = [], []
        for i, s in enumerate(scores):
            if masked:
                s = jnp.where(gaps(bq) >= j * KEYS - iq * bq, s, HIDDEN)
            old = top_s[i : i + 1, :]
            top = jnp.maximum(old, s.max(axis=0, keepdims=True))
            top_s[i : i + 1, :] = top
            weights.append(jnp.exp2((s - top) * e).astype(BF16))
            keeps.append(jnp.exp2((old - top) * e))
        for i, (p, keep) in enumerate(zip(weights, keeps)):
            mix_s[i] = mix_s[i] * keep + _dot(values, p, 1, 0)

    last = (iq * bq) // KEYS
    lax.fori_loop(0, last, lambda j, _: block(j, False), None)
    block(last, True)
    for i, heads in enumerate(pieces):
        total = mix_s[i, HEAD : HEAD + 1, :]
        out = (mix_s[i, :HEAD, :] * (1 / total)).T.astype(BF16)
        lse = top_s[i : i + 1, :] * SCALE + jnp.log(total)
        for at, n in enumerate(heads):
            out_ref[:, lanes(n)] = out[at * bq : (at + 1) * bq, :]
            lse_ref[0, n : n + 1, :] = lse[:, at * bq : (at + 1) * bq]


def attend(q, k, v, cos, sin):
    tokens = q.shape[0]
    kv = k.shape[1] // HEAD
    bq = 256
    queries = pl.BlockSpec((bq, SPAN), lambda h, i: (i, h))
    keys = pl.BlockSpec((tokens, HEAD), lambda h, i: (0, h))
    table = pl.BlockSpec((tokens, HEAD), lambda h, i: (0, 0))
    count = len(strips(bq))
    return pl.pallas_call(
        forward,
        grid=(kv, tokens // bq),
        in_specs=[queries, keys, keys, table, table],
        out_specs=[queries, pl.BlockSpec((1, SPAN // HEAD, bq), lambda h, i: (h, 0, i)), queries, keys],
        out_shape=[jax.ShapeDtypeStruct(q.shape, BF16), jax.ShapeDtypeStruct((kv, SPAN // HEAD, tokens), F32),
                   jax.ShapeDtypeStruct(q.shape, BF16), jax.ShapeDtypeStruct(k.shape, BF16)],
        scratch_shapes=[pltpu.VMEM((count, STRIP), F32), pltpu.VMEM((count, HEAD + 8, STRIP), F32)],
        compiler_params=pltpu.CompilerParams(dimension_semantics=("parallel", "arbitrary"), vmem_limit_bytes=56 * MIB),
        cost_estimate=pl.CostEstimate(flops=4 * q.size * tokens, transcendentals=q.size * tokens // HEAD, bytes_accessed=8 * q.size),
        name="attend",
    )(q, k, v, cos, sin)


def backward(q_ref, k_ref, v_ref, do_ref, out_ref, lse_ref, cos_ref, sin_ref, dq_ref, dk_ref, dv_ref, dq_s, dk_s, dv_s, delta_s, pick_s):
    bq = q_ref.shape[0]
    iq = pl.program_id(1)
    e = SCALE * LOG2E
    pieces = strips(bq)

    @pl.when(iq == 0)
    def _():
        dk_s[...] = jnp.zeros_like(dk_s)
        dv_s[...] = jnp.zeros_like(dv_s)
        of = lax.broadcasted_iota(jnp.int32, pick_s.shape, 0) // HEAD
        pick_s[...] = jnp.where(of == lax.broadcasted_iota(jnp.int32, pick_s.shape, 1), 1.0, 0.0).astype(BF16)

    product = do_ref[...].astype(F32) * out_ref[...].astype(F32)
    high = product.astype(BF16)
    low = (product - high.astype(F32)).astype(BF16)
    delta_s[...] = (_dot(high, pick_s[...], 1, 0) + _dot(low, pick_s[...], 1, 0)).T
    dq_s[...] = jnp.zeros_like(dq_s)

    def block(j, masked):
        keys = pl.ds(pl.multiple_of(j * KEYS, KEYS), KEYS)
        qs = [stacked(q_ref, heads) for heads in pieces]
        dos = [stacked(do_ref, heads) for heads in pieces]
        scores = [_dot(k_ref[keys, :], x, 1, 1) for x in qs]
        dps = [_dot(v_ref[keys, :], x, 1, 1) for x in dos]
        for i, heads in enumerate(pieces):
            p = jnp.exp2(scores[i] * e - row(lse_ref.at[0], heads) * LOG2E)
            if masked:
                p = jnp.where(gaps(bq) >= j * KEYS - iq * bq, p, 0.0)
            ds = (p * (dps[i] - row(delta_s, heads))).astype(BF16)
            dv_s[keys, :] += _dot(p.astype(BF16), dos[i], 1, 0)
            dk_s[keys, :] += _dot(ds, qs[i], 1, 0)
            dq_s[i] += _dot(k_ref[keys, :].T, ds, 1, 0)

    last = (iq * bq) // KEYS
    lax.fori_loop(0, last, lambda j, _: block(j, False), None)
    block(last, True)
    here = pl.ds(pl.multiple_of(iq * bq, bq), bq)
    cos, sin = cos_ref[here, :], sin_ref[here, :]
    for i, heads in enumerate(pieces):
        dq = (dq_s[i] * SCALE).T
        for at, n in enumerate(heads):
            dq_ref[:, lanes(n)] = turn_back(dq[at * bq : (at + 1) * bq, :], cos, sin)

    @pl.when(iq == pl.num_programs(1) - 1)
    def _():
        dk_ref[...] = turn_back(dk_s[...] * SCALE, cos_ref[...], sin_ref[...])
        dv_ref[...] = dv_s[...].astype(BF16)


MESH = pl.DeviceIdType.MESH
RING = 4
PARTS = 6
STAGES = 6
GROUP = 4
GROUP_ROWS = 40
OWN_ROWS = 10
TALL, WIDE, MORE = "tall", "wide", "more"
TILES = 5
PADDED = 16
FULL = slice(None)


def place():
    me = lax.axis_index("dp")
    chip = me // 2
    return (chip // RING**2, chip // RING % RING, chip % RING), me % 2


def flip(c, m):
    return c + 1 - 2 * (c % 2) if m == 1 else RING - 1 - c


def masks(p):
    return (1, RING - 1) if p < PARTS // 2 else (RING - 1, 1)


def order(p):
    return [(p + i) % 3 for i in range(3)]


def device(xyz, core):
    return {"dp": ((xyz[0] * RING + xyz[1]) * RING + xyz[2]) * 2 + core}


def partner(xyz, core, dim, m):
    to = list(xyz)
    to[dim] = flip(to[dim], m)
    return device(to, core)


def in_group(xyz, q):
    return device((*xyz[:2], xyz[2] // 2 * 2 + q // 2), q % 2)


def enter(xyz, core):
    barrier = pltpu.get_barrier_semaphore()
    others = [partner(xyz, core, dim, m) for dim in range(3) for m in masks(0)]
    others += [device(xyz, 1 - core), partner(xyz, 1 - core, 2, 1)]
    for to in others:
        pl.semaphore_signal(barrier, inc=1, device_id=to, device_id_type=MESH)
    pl.semaphore_wait(barrier, len(others))


def remote(src, dst, send, recv, to):
    pltpu.make_async_remote_copy(src_ref=src, dst_ref=dst, send_sem=send, recv_sem=recv, device_id=to, device_id_type=MESH).start()


def await_bytes(ref, sem):
    pltpu.make_async_copy(ref, ref, sem).wait()


def spots(kind, p):
    if kind == TALL:
        return [((p % 3, FULL, pl.ds(p // 3 * TILES * HEAD, TILES * HEAD)), ())]
    if kind == WIDE:
        return [((FULL, FULL, lanes(p)), ())]
    some = [((FULL, FULL, lanes(p)), (pl.ds(0, TILES),))]
    return some + [((p, FULL, lanes(PARTS)), (TILES,))] if p < TILES else some


def cuts(kind, hbm, vmem, core):
    if kind == TALL:
        return [(hbm[0].at[:, :, :, core], vmem)]
    pairs = []
    for z in range(RING):
        for i, one in enumerate(hbm):
            at, size = (0, PARTS * HEAD) if i == 0 else (PARTS * HEAD, HEAD)
            c = pl.ds(pl.multiple_of((core * 2 + z % 2) * size, HEAD), size)
            pairs.append((one.at[:, :, z // 2, :, :, c], vmem.at[:, :, z, :, :, pl.ds(at, size)]))
    return pairs


def some(half, k):
    zeros = (0,) * ((k - 1) // 2)
    return half.at[(*zeros, pl.ds(0, 2))] if k % 2 else half.at[(*zeros, 0)]


def taker(refs):
    refs = list(refs)
    return lambda count: [refs.pop(0) for _ in range(count)]


def count_in(kind):
    return 2 if kind == MORE else 1


def flat_refs(kinds, take):
    return [take(1)[0] if kind != TALL else None for kind in kinds]


class Scatter:
    def __init__(self, kinds, ins, outs, scratch):
        n = len(kinds)
        take, given = taker(scratch), taker(ins)
        self.kinds, self.outs = kinds, outs
        self.ins = [given(count_in(kind)) for kind in kinds]
        self.own, self.beside = take(n), take(n)
        self.got = [take(STAGES) for _ in kinds]
        self.flat, self.cut, self.gathered = (flat_refs(kinds, take) for _ in range(3))
        self.load_sem, self.core_send, self.core_recv, self.send_sem, self.recv_sem, self.fix_send, self.fix_recv = take(7)
        self.xyz, self.core = place()

    def start(self):
        enter(self.xyz, self.core)
        core = self.core
        for j, kind in enumerate(self.kinds):
            for src, dst in cuts(kind, self.ins[j], self.beside[j], 1 - core):
                remote(src, dst, self.core_send.at[j], self.core_recv.at[j], device(self.xyz, 1 - core))
            for src, dst in cuts(kind, self.ins[j], self.own[j], core):
                pltpu.make_async_copy(src, dst, self.load_sem.at[j]).start()

    def each(self, j, k, p, slot, cs, ct):
        dims, g = order(p), self.got[j]
        c = [self.xyz[d] for d in dims]
        a, m = masks(p)
        way = (k - 1) // 2
        free = [None, cs, ct]
        where = []
        for i in range(3):
            if i > way:
                where.append(free[i])
            elif i < way:
                where.append(c[i])
            elif k % 2:
                where.append(flip(c[i], a) if slot == 0 else flip(flip(c[i], a), m))
            else:
                where.append(flip(c[i], m))
        index = [None] * 3
        for d, one in zip(dims, where):
            index[d] = one
        others = [index[d] for d in range(3) if d != dims[0]]
        terms = []
        for stage in range(1, k):
            i = (stage - 1) // 2
            tail = others if i == 0 else where[i + 1 :]
            lead = [1 if stage == k - 1 and k % 2 == 0 else 0] if stage % 2 else []
            terms.append((g[stage - 1], (p, *lead, *tail)))
        return tuple(index), terms

    def totals(self, j, p, index, terms):
        for inside, among in spots(self.kinds[j], p):
            total = self.own[j][(*index, *inside)].astype(F32) + self.beside[j][(*index, *inside)].astype(F32)
            for ref, where in terms:
                total = total + ref[(*where, *among)].astype(F32)
            yield inside, total

    def stage(self, j, k):
        own, g = self.own[j], self.got[j]
        if k == 1:
            await_bytes(own, self.load_sem.at[j])
            await_bytes(self.beside[j], self.core_recv.at[j])
        else:
            await_bytes(some(own, k - 1), self.recv_sem.at[j, k - 2])
        if k > STAGES:
            self.last(j, k)
            return
        slots = range(1 + k % 2)

        def put(cs, ct):
            for p in range(PARTS):
                for slot in slots:
                    index, terms = self.each(j, k, p, slot, cs, ct)
                    for inside, total in self.totals(j, p, index, terms):
                        own[(*index, *inside)] = total.astype(BF16)

        way = (k - 1) // 2
        if way == 0:
            pl.loop(0, RING**2)(lambda i: put(i // RING, i % RING))
        elif way == 1:
            pl.loop(0, RING)(lambda i: put(None, i))
        else:
            put(None, None)
        for p in range(PARTS):
            to = partner(self.xyz, self.core, order(p)[way], masks(p)[1 - k % 2])
            for slot in slots:
                index, _ = self.each(j, k, p, slot, FULL, FULL)
                lead = ((p, slot) if k % 2 else (p,)) + (FULL,) * (2 - way)
                for inside, among in spots(self.kinds[j], p):
                    dst = g[k - 1].at[(*lead, *among)]
                    remote(own.at[(*index, *inside)], dst, self.send_sem.at[j, k - 1], self.recv_sem.at[j, k - 1], to)

    def last(self, j, k):
        kind, flat, cut, gathered = self.kinds[j], self.flat[j], self.cut[j], self.gathered[j]
        for p in range(PARTS):
            for inside, total in self.totals(j, p, *self.each(j, k, p, 0, None, None)):
                if kind == TALL:
                    self.outs[j][inside] = total.astype(BF16)
                    continue
                first = 0 if inside[0] == FULL else inside[0]
                flat[8 * first : 8 * first + total.size // HEAD, inside[2]] = total.reshape(-1, HEAD)
        if kind == TALL:
            return
        mine = self.xyz[2] % 2 * 2 + self.core
        for q in range(GROUP):
            cut[q, 0:OWN_ROWS, :] = flat[OWN_ROWS * q : OWN_ROWS * (q + 1), :].astype(BF16)
        for q in range(GROUP):
            @pl.when(mine != q)
            def _():
                remote(cut.at[q], gathered.at[mine], self.fix_send.at[j], self.fix_recv.at[j], in_group(self.xyz, q))

            @pl.when(mine == q)
            def _():
                gathered[q] = cut[q]

    def waves(self):
        n = len(self.kinds)
        return [[(j, wave - j + 1) for j in reversed(range(n)) if 1 <= wave - j + 1 <= STAGES + 1] for wave in range(n + STAGES)]

    def run(self, wave):
        for j, k in wave:
            self.stage(j, k)

    def finish(self):
        for j, kind in enumerate(self.kinds):
            await_bytes(self.beside[j], self.core_send.at[j])
            for k in range(STAGES):
                await_bytes(some(self.own[j], k + 1), self.send_sem.at[j, k])
            if kind != TALL:
                three = self.gathered[j].at[pl.ds(0, GROUP - 1)]
                await_bytes(three, self.fix_recv.at[j])
                await_bytes(three, self.fix_send.at[j])
                self.outs[j][...] = self.gathered[j][...]


WIDE_SHAPE = (RING, RING, 2, TILES, 8, 3072)
SMALL_SHAPE = (RING, RING, 2, TILES, 8, 512)
TALL_SHAPE = (RING, RING, RING, 2, 3, 8, 1280)


def width(kind):
    return (PARTS + 1 if kind == MORE else PARTS) * HEAD


def halves(kinds):
    return [pltpu.VMEM((RING, RING, RING) + ((3, 8, 1280) if kind == TALL else (TILES, 8, width(kind))), BF16) for kind in kinds]


def pieces_of(kind, *lead):
    return pltpu.VMEM((PARTS, *lead) + ((8, TILES * HEAD) if kind == TALL else (TILES + (kind == MORE), 8, HEAD)), BF16)


def wide_scratch(kinds, rows, dtype):
    return [pltpu.VMEM((*rows, width(kind)), dtype) for kind in kinds if kind != TALL]


def own_shapes(kinds):
    return [jax.ShapeDtypeStruct((3, 8, 1280) if kind == TALL else (GROUP, PADDED, width(kind)), BF16) for kind in kinds]


def semaphores(n):
    sem = pltpu.SemaphoreType.DMA
    return [sem((n,))] * 3 + [sem((n, STAGES))] * 2 + [sem((n,))] * 2


def scatter_scratch(kinds):
    scratch = halves(kinds) * 2
    for kind in kinds:
        for lead in ((2, RING, RING), (RING, RING), (2, RING), (RING,), (2,), ()):
            scratch.append(pieces_of(kind, *lead))
    scratch += wide_scratch(kinds, (GROUP_ROWS,), F32)
    scratch += wide_scratch(kinds, (GROUP, PADDED), BF16) * 2
    return scratch + semaphores(len(kinds))


def scatter_inputs(kinds, arrays):
    ins = []
    for kind, given in zip(kinds, arrays):
        if kind == TALL:
            ins.append(given.reshape(TALL_SHAPE))
        elif kind == MORE:
            ins += [given[0].reshape(WIDE_SHAPE), given[1].reshape(SMALL_SHAPE)]
        else:
            ins.append(given.reshape(WIDE_SHAPE))
    return ins


def talks(number, mib=63):
    return pltpu.CompilerParams(collective_id=number, has_side_effects=True, vmem_limit_bytes=mib * MIB)


ANYWHERE, ON_CHIP = pl.BlockSpec(memory_space=pl.ANY), pl.BlockSpec(memory_space=pltpu.VMEM)


def scatter(kinds, arrays, number):
    ins, outs = scatter_inputs(kinds, arrays), own_shapes(kinds)

    def kernel(*refs):
        take = taker(refs)
        sums = Scatter(kinds, take(len(ins)), take(len(outs)), take(len(scatter_scratch(kinds))))
        sums.start()
        for wave in sums.waves():
            sums.run(wave)
        sums.finish()

    return pl.pallas_call(
        kernel,
        out_shape=outs,
        in_specs=[ANYWHERE] * len(ins),
        out_specs=[ON_CHIP] * len(outs),
        scratch_shapes=scatter_scratch(kinds),
        compiler_params=talks(number),
        name=f"scatter{number}",
    )(*ins)


class Gather:
    def __init__(self, kinds, ins, outs, scratch):
        n = len(kinds)
        take, given = taker(scratch), taker(outs)
        self.kinds, self.ins = kinds, ins
        self.outs = [given(count_in(kind)) for kind in kinds]
        self.full = take(n)
        self.flat, self.came = (flat_refs(kinds, take) for _ in range(2))
        self.store_sem, self.core_send, self.core_recv, self.send_sem, self.recv_sem, self.fix_send, self.fix_recv = take(7)
        self.xyz, self.core = place()

    def start(self):
        enter(self.xyz, self.core)
        mine = self.xyz[2] % 2 * 2 + self.core
        for j, kind in enumerate(self.kinds):
            if kind == TALL:
                continue
            for q in range(GROUP):
                @pl.when(mine != q)
                def _():
                    remote(self.ins[j].at[q], self.came[j].at[mine], self.fix_send.at[j], self.fix_recv.at[j], in_group(self.xyz, q))

                @pl.when(mine == q)
                def _():
                    self.came[j][q] = self.ins[j][q]

    def first(self, j):
        kind, o, flat, came = self.kinds[j], self.full[j], self.flat[j], self.came[j]
        if kind == TALL:
            o[self.xyz] = self.ins[j][...]
            return
        await_bytes(came.at[pl.ds(0, GROUP - 1)], self.fix_recv.at[j])
        for q in range(GROUP):
            flat[OWN_ROWS * q : OWN_ROWS * (q + 1), :] = came[q, 0:OWN_ROWS, :].astype(F32)
        for t in range(TILES):
            o[(*self.xyz, t)] = flat[8 * t : 8 * t + 8, :].astype(BF16)

    def stage(self, j, k):
        o = self.full[j]
        if k == STAGES:
            self.first(j)
        else:
            await_bytes(some(o, k + 1), self.recv_sem.at[j, k])
        if k == 0:
            for dst, src in cuts(self.kinds[j], self.outs[j], o, self.core):
                remote(src, dst, self.core_send.at[j], self.core_recv.at[j], device(self.xyz, 1 - self.core))
                pltpu.make_async_copy(src, dst, self.store_sem.at[j]).start()
            return
        way = (k - 1) // 2
        for p in range(PARTS):
            dims = order(p)
            mine = self.xyz[dims[way]]
            held = (mine, flip(mine, masks(p)[1])) if k % 2 else (mine,)
            to = partner(self.xyz, self.core, dims[way], masks(p)[1 - k % 2])
            for one in held:
                index = [FULL] * 3
                for i in range(way):
                    index[dims[i]] = self.xyz[dims[i]]
                index[dims[way]] = one
                for inside, _ in spots(self.kinds[j], p):
                    view = o.at[(*index, *inside)]
                    remote(view, view, self.send_sem.at[j, k - 1], self.recv_sem.at[j, k - 1], to)

    def waves(self):
        n = len(self.kinds)
        return [[(j, STAGES - wave + j) for j in range(n) if 0 <= STAGES - wave + j <= STAGES] for wave in range(n + STAGES)]

    run = Scatter.run

    def finish(self):
        for j, kind in enumerate(self.kinds):
            for k in range(1, STAGES + 1):
                await_bytes(some(self.full[j], k), self.send_sem.at[j, k - 1])
            if kind != TALL:
                await_bytes(self.came[j].at[pl.ds(0, GROUP - 1)], self.fix_send.at[j])
            for sem in (self.core_send, self.core_recv, self.store_sem):
                await_bytes(self.full[j], sem.at[j])


def gather_scratch(kinds):
    scratch = halves(kinds)
    scratch += wide_scratch(kinds, (GROUP_ROWS,), F32)
    scratch += wide_scratch(kinds, (GROUP, PADDED), BF16)
    return scratch + semaphores(len(kinds))


def whole_shapes(kinds):
    shapes = []
    for kind in kinds:
        shapes.append(TALL_SHAPE if kind == TALL else WIDE_SHAPE)
        if kind == MORE:
            shapes.append(SMALL_SHAPE)
    return [jax.ShapeDtypeStruct(shape, BF16) for shape in shapes]


def gather(kinds, arrays, number):
    outs = whole_shapes(kinds)

    def kernel(*refs):
        take = taker(refs)
        new = Gather(kinds, take(len(kinds)), take(len(outs)), take(len(gather_scratch(kinds))))
        new.start()
        for wave in new.waves():
            new.run(wave)
        new.finish()

    return pl.pallas_call(
        kernel,
        out_shape=outs,
        in_specs=[ON_CHIP] * len(kinds),
        out_specs=[ANYWHERE] * len(outs),
        scratch_shapes=gather_scratch(kinds),
        compiler_params=talks(number, 20),
        name=f"gather{number}",
    )(*arrays)


def attend_bwd(q, k, v, d_out, out, lse, cos, sin, kinds, arrays, number):
    tokens = q.shape[0]
    kv = k.shape[1] // HEAD
    bq = 128
    steps = tokens // bq
    ins, sums_out = scatter_inputs(kinds, arrays), own_shapes(kinds)
    queries = pl.BlockSpec((bq, SPAN), lambda h, i: (i, h))
    keys = pl.BlockSpec((tokens, HEAD), lambda h, i: (0, h))
    table = pl.BlockSpec((tokens, HEAD), lambda h, i: (0, 0))
    count = len(strips(bq))
    own_scratch = [pltpu.VMEM((count, HEAD, STRIP), F32), pltpu.VMEM((tokens, HEAD), F32), pltpu.VMEM((tokens, HEAD), F32),
                   pltpu.VMEM((HEAD, bq), F32), pltpu.VMEM((SPAN, HEAD), BF16)]

    def kernel(*refs):
        take = taker(refs)
        first = take(8)
        ready = take(len(ins))
        last = take(3)
        sums_refs = take(len(sums_out))
        own = take(len(own_scratch))
        sums = Scatter(kinds, ready, sums_refs, take(len(scatter_scratch(kinds))))
        step = pl.program_id(0) * steps + pl.program_id(1)
        waves = sums.waves()
        at_step = {}
        for i, wave in enumerate(waves):
            at_step.setdefault(min(FIRST + i * APART // 4, kv * steps - 1), []).append(wave)

        @pl.when(step == 0)
        def _():
            sums.start()

        backward(*first, *last, *own)
        for n, some in at_step.items():
            @pl.when(step == n)
            def _():
                for wave in some:
                    sums.run(wave)

        @pl.when(step == kv * steps - 1)
        def _():
            sums.finish()

    return pl.pallas_call(
        kernel,
        grid=(kv, steps),
        in_specs=[queries, keys, keys, queries, queries, pl.BlockSpec((1, SPAN // HEAD, bq), lambda h, i: (h, 0, i)), table, table]
        + [ANYWHERE] * len(ins),
        out_specs=[queries, keys, keys] + [ON_CHIP] * len(sums_out),
        out_shape=[jax.ShapeDtypeStruct(one.shape, BF16) for one in (q, k, v)] + sums_out,
        scratch_shapes=own_scratch + scatter_scratch(kinds),
        compiler_params=talks(number),
        name=f"attend_bwd{number}",
    )(q, k, v, d_out, out, lse, cos, sin, *ins)


FIRST, APART = 1, 6


def matmul(a, w):
    return jnp.dot(a, w, preferred_element_type=F32).astype(BF16)


def normed(h):
    wide = h.astype(F32)
    scale = lax.rsqrt(jnp.mean(wide**2, -1, keepdims=True) + 1e-6)
    return (wide * scale).astype(BF16)


def projections(a, wq, wk, wv):
    return matmul(a, wq), matmul(a, wk), matmul(a, wv)


def tail(h, mixed, wo, w_gate, w_up, w_down):
    h = h + matmul(mixed, wo)
    b = normed(h)
    gate = jnp.dot(b, w_gate, preferred_element_type=F32)
    up = jnp.dot(b, w_up, preferred_element_type=F32)
    return h + matmul((jax.nn.silu(gate) * up).astype(BF16), w_down)


def adamw(w, m, v, g):
    m = 0.9 * m + 0.1 * g
    v = 0.95 * v + 0.05 * g * g
    step = m * lax.rsqrt(v + 1e-8) + 0.1 * w
    return (w - 0.02 * step).astype(BF16), m, v


def from_quarters(got):
    return got[:, :OWN_ROWS].reshape(2, 2, OWN_ROWS, -1).transpose(2, 1, 0, 3).reshape(OWN_ROWS, -1)


def to_quarters(block):
    cut = block.reshape(OWN_ROWS, 2, 2, -1).transpose(2, 1, 0, 3).reshape(GROUP, OWN_ROWS, -1)
    return jnp.pad(cut, ((0, 0), (0, PADDED - OWN_ROWS), (0, 0)))


LATE, EARLY = (WIDE, WIDE, TALL), (MORE, TALL)


def solution(mesh):
    def step(x, dy, *arrays):
        weights, m, v = (arrays[i : i + 7] for i in (0, 7, 14))
        w = {name: one[0] for name, one in zip(NAMES, weights, strict=True)}
        first, second = (dict(zip(NAMES, some, strict=True)) for some in (m, v))
        cos, sin = angles(x.shape[1])
        h = x[0]
        (q, k, val), back = jax.vjp(functools.partial(projections, normed(h)), w["wq"], w["wk"], w["wv"])
        mixed, lse, q, k = attend(q, k, val, cos, sin)
        _, tail_back = jax.vjp(functools.partial(tail, h), mixed, w["wo"], w["w_gate"], w["w_up"], w["w_down"])
        by_mixed, g_o, g_gate, g_up, g_down = tail_back(dy[0])
        dq, dk, dv, s_gate, s_up, s_down = attend_bwd(q, k, val, by_mixed, mixed, lse, cos, sin, LATE, [g_gate, g_up, g_down], 1)
        g_q, g_k, g_v = back((dq, dk, dv))
        s_q, s_o = scatter(EARLY, [(g_q, jnp.concatenate([g_k, g_v], 1)), g_o], 2)

        me = lax.axis_index("dp")
        new = {}

        def update(name, g):
            one = first[name]
            rows = one.shape[1]
            own = lax.dynamic_slice_in_dim(w[name], me * rows, rows, 0).astype(F32)
            new[name] = adamw(own, one[0], second[name][0], g.astype(F32))
            return new[name][0]

        def update_tall(name, g):
            return update(name, g.reshape(-1, g.shape[2])).reshape(g.shape)

        update_wide = lambda name, g: to_quarters(update(name, from_quarters(g)))
        late = [update_wide("w_gate", s_gate), update_wide("w_up", s_up), update_tall("w_down", s_down)]
        gate, up, down = gather(LATE, late, 3)
        kv = from_quarters(s_q[:, :, PARTS * HEAD :])
        half = kv.shape[1] // 2
        kv = to_quarters(jnp.concatenate([update("wk", kv[:, :half]), update("wv", kv[:, half:])], 1))
        early = [jnp.concatenate([update_wide("wq", s_q[:, :, : PARTS * HEAD]), kv], 2), update_tall("wo", s_o)]
        q, kv, o = gather(EARLY, early, 4)
        kv = kv.reshape(-1, kv.shape[-1])
        whole = {"wq": q, "wk": kv[:, :half], "wv": kv[:, half:], "wo": o, "w_gate": gate, "w_up": up, "w_down": down}
        moments = [new[name][i][None] for i in (1, 2) for name in NAMES]
        return (*(whole[name].reshape(one.shape) for name, one in zip(NAMES, weights, strict=True)), *moments)

    states, all_of, cut = P(("rep", "dp"), None, None), P(None, None, None), P(None, "dp", None)
    return jax.shard_map(
        step,
        mesh=mesh,
        in_specs=(states, states) + (all_of,) * 7 + (cut,) * 14,
        out_specs=(P("rep", None, None),) * 7 + (P("rep", "dp", None),) * 14,
        check_vma=False,
    )
```

```python
import functools

import jax
import jax.numpy as jnp
from jax import lax
from jax.experimental import pallas as pl
from jax.experimental.pallas import tpu as pltpu
from jax.sharding import PartitionSpec as P

NEG = -1e30
HIDDEN = 2 * NEG
LOG2E = 1.4426950408889634
HEAD = 128
THETA = 10000
SPAN = 12 * HEAD
SCALE = HEAD**-0.5
STRIP = 512
KEYS = 256
NAMES = ("wq", "wk", "wv", "wo", "w_gate", "w_up", "w_down")
MIB = 2**20
F32, BF16 = jnp.float32, jnp.bfloat16


def _dot(a, b, ca, cb):
    return lax.dot_general(a, b, (((ca,), (cb,)), ((), ())), preferred_element_type=F32)


def angles(tokens):
    half = HEAD // 2
    angle = jnp.arange(tokens, dtype=F32)[:, None] * THETA ** (-jnp.arange(half, dtype=F32) / half)
    cos, sin = jnp.cos(angle), jnp.sin(angle)
    return jnp.concatenate([cos, cos], 1), jnp.concatenate([-sin, sin], 1)


def swapped(t):
    return pltpu.roll(t, HEAD // 2, 1)


def turn(t, cos, sin):
    t = t.astype(F32)
    return (t * cos + swapped(t) * sin).astype(BF16)


def turn_back(t, cos, sin):
    t = t.astype(BF16).astype(F32)
    return (t * cos + swapped(t * sin)).astype(BF16)


def lanes(n):
    return slice(n * HEAD, (n + 1) * HEAD)


def strips(bq):
    per = STRIP // bq
    return [range(n, n + per) for n in range(0, SPAN // HEAD, per)]


def stacked(ref, heads):
    return jnp.concatenate([ref[:, lanes(n)] for n in heads], axis=0)


def row(ref, heads):
    return jnp.concatenate([ref[n : n + 1, :] for n in heads], axis=1)


def gaps(bq):
    shape = (KEYS, STRIP)
    return lax.rem(lax.broadcasted_iota(jnp.int32, shape, 1), bq) - lax.broadcasted_iota(jnp.int32, shape, 0)


def forward(q_ref, k_ref, v_ref, cos_ref, sin_ref, out_ref, lse_ref, qt_ref, kt_ref, top_s, mix_s):
    bq = q_ref.shape[0]
    iq = pl.program_id(1)
    e = SCALE * LOG2E

    @pl.when(iq == 0)
    def _():
        kt_ref[...] = turn(k_ref[...], cos_ref[...], sin_ref[...])

    here = pl.ds(pl.multiple_of(iq * bq, bq), bq)
    cos, sin = cos_ref[here, :], sin_ref[here, :]
    for n in range(SPAN // HEAD):
        qt_ref[:, lanes(n)] = turn(q_ref[:, lanes(n)], cos, sin)
    top_s[...] = jnp.full_like(top_s, NEG)
    mix_s[...] = jnp.zeros_like(mix_s)
    ones = jnp.ones((8, KEYS), BF16)
    pieces = strips(bq)

    def block(j, masked):
        keys = pl.ds(pl.multiple_of(j * KEYS, KEYS), KEYS)
        values = jnp.concatenate([v_ref[keys, :].T, ones], axis=0)
        scores = [_dot(kt_ref[keys, :], stacked(qt_ref, heads), 1, 1) for heads in pieces]
        weights, keeps = [], []
        for i, s in enumerate(scores):
            if masked:
                s = jnp.where(gaps(bq) >= j * KEYS - iq * bq, s, HIDDEN)
            old = top_s[i : i + 1, :]
            top = jnp.maximum(old, s.max(axis=0, keepdims=True))
            top_s[i : i + 1, :] = top
            weights.append(jnp.exp2((s - top) * e).astype(BF16))
            keeps.append(jnp.exp2((old - top) * e))
        for i, (p, keep) in enumerate(zip(weights, keeps)):
            mix_s[i] = mix_s[i] * keep + _dot(values, p, 1, 0)

    last = (iq * bq) // KEYS
    lax.fori_loop(0, last, lambda j, _: block(j, False), None)
    block(last, True)
    for i, heads in enumerate(pieces):
        total = mix_s[i, HEAD : HEAD + 1, :]
        out = (mix_s[i, :HEAD, :] * (1 / total)).T.astype(BF16)
        lse = top_s[i : i + 1, :] * SCALE + jnp.log(total)
        for at, n in enumerate(heads):
            out_ref[:, lanes(n)] = out[at * bq : (at + 1) * bq, :]
            lse_ref[0, n : n + 1, :] = lse[:, at * bq : (at + 1) * bq]


def attend(q, k, v, cos, sin):
    tokens = q.shape[0]
    kv = k.shape[1] // HEAD
    bq = 256
    queries = pl.BlockSpec((bq, SPAN), lambda h, i: (i, h))
    keys = pl.BlockSpec((tokens, HEAD), lambda h, i: (0, h))
    table = pl.BlockSpec((tokens, HEAD), lambda h, i: (0, 0))
    count = len(strips(bq))
    return pl.pallas_call(
        forward,
        grid=(kv, tokens // bq),
        in_specs=[queries, keys, keys, table, table],
        out_specs=[queries, pl.BlockSpec((1, SPAN // HEAD, bq), lambda h, i: (h, 0, i)), queries, keys],
        out_shape=[jax.ShapeDtypeStruct(q.shape, BF16), jax.ShapeDtypeStruct((kv, SPAN // HEAD, tokens), F32),
                   jax.ShapeDtypeStruct(q.shape, BF16), jax.ShapeDtypeStruct(k.shape, BF16)],
        scratch_shapes=[pltpu.VMEM((count, STRIP), F32), pltpu.VMEM((count, HEAD + 8, STRIP), F32)],
        compiler_params=pltpu.CompilerParams(dimension_semantics=("parallel", "arbitrary"), vmem_limit_bytes=56 * MIB),
        cost_estimate=pl.CostEstimate(flops=4 * q.size * tokens, transcendentals=q.size * tokens // HEAD, bytes_accessed=8 * q.size),
        name="attend",
    )(q, k, v, cos, sin)


def backward(q_ref, k_ref, v_ref, do_ref, out_ref, lse_ref, cos_ref, sin_ref, dq_ref, dk_ref, dv_ref, dq_s, dk_s, dv_s, delta_s, pick_s):
    bq = q_ref.shape[0]
    iq = pl.program_id(1)
    e = SCALE * LOG2E
    pieces = strips(bq)

    @pl.when(iq == 0)
    def _():
        dk_s[...] = jnp.zeros_like(dk_s)
        dv_s[...] = jnp.zeros_like(dv_s)
        of = lax.broadcasted_iota(jnp.int32, pick_s.shape, 0) // HEAD
        pick_s[...] = jnp.where(of == lax.broadcasted_iota(jnp.int32, pick_s.shape, 1), 1.0, 0.0).astype(BF16)

    product = do_ref[...].astype(F32) * out_ref[...].astype(F32)
    high = product.astype(BF16)
    low = (product - high.astype(F32)).astype(BF16)
    delta_s[...] = (_dot(high, pick_s[...], 1, 0) + _dot(low, pick_s[...], 1, 0)).T
    dq_s[...] = jnp.zeros_like(dq_s)

    def block(j, masked):
        keys = pl.ds(pl.multiple_of(j * KEYS, KEYS), KEYS)
        qs = [stacked(q_ref, heads) for heads in pieces]
        dos = [stacked(do_ref, heads) for heads in pieces]
        scores = [_dot(k_ref[keys, :], x, 1, 1) for x in qs]
        dps = [_dot(v_ref[keys, :], x, 1, 1) for x in dos]
        for i, heads in enumerate(pieces):
            p = jnp.exp2(scores[i] * e - row(lse_ref.at[0], heads) * LOG2E)
            if masked:
                p = jnp.where(gaps(bq) >= j * KEYS - iq * bq, p, 0.0)
            ds = (p * (dps[i] - row(delta_s, heads))).astype(BF16)
            dv_s[keys, :] += _dot(p.astype(BF16), dos[i], 1, 0)
            dk_s[keys, :] += _dot(ds, qs[i], 1, 0)
            dq_s[i] += _dot(k_ref[keys, :].T, ds, 1, 0)

    last = (iq * bq) // KEYS
    lax.fori_loop(0, last, lambda j, _: block(j, False), None)
    block(last, True)
    here = pl.ds(pl.multiple_of(iq * bq, bq), bq)
    cos, sin = cos_ref[here, :], sin_ref[here, :]
    for i, heads in enumerate(pieces):
        dq = (dq_s[i] * SCALE).T
        for at, n in enumerate(heads):
            dq_ref[:, lanes(n)] = turn_back(dq[at * bq : (at + 1) * bq, :], cos, sin)

    @pl.when(iq == pl.num_programs(1) - 1)
    def _():
        dk_ref[...] = turn_back(dk_s[...] * SCALE, cos_ref[...], sin_ref[...])
        dv_ref[...] = dv_s[...].astype(BF16)


MESH = pl.DeviceIdType.MESH
RING = 4
PARTS = 6
STAGES = 6
GROUP = 4
GROUP_ROWS = 40
OWN_ROWS = 10
TALL, WIDE, MORE = "tall", "wide", "more"
TILES = 5
PADDED = 16
FULL = slice(None)


def place():
    me = lax.axis_index("dp")
    chip = me // 2
    return (chip // RING**2, chip // RING % RING, chip % RING), me % 2


def flip(c, m):
    return c + 1 - 2 * (c % 2) if m == 1 else RING - 1 - c


def masks(p):
    return (1, RING - 1) if p < PARTS // 2 else (RING - 1, 1)


def order(p):
    return [(p + i) % 3 for i in range(3)]


def device(xyz, core):
    return {"dp": ((xyz[0] * RING + xyz[1]) * RING + xyz[2]) * 2 + core}


def partner(xyz, core, dim, m):
    to = list(xyz)
    to[dim] = flip(to[dim], m)
    return device(to, core)


def in_group(xyz, q):
    return device((*xyz[:2], xyz[2] // 2 * 2 + q // 2), q % 2)


def enter(xyz, core):
    barrier = pltpu.get_barrier_semaphore()
    others = [partner(xyz, core, dim, m) for dim in range(3) for m in masks(0)]
    others += [device(xyz, 1 - core), partner(xyz, 1 - core, 2, 1)]
    for to in others:
        pl.semaphore_signal(barrier, inc=1, device_id=to, device_id_type=MESH)
    pl.semaphore_wait(barrier, len(others))


def remote(src, dst, send, recv, to):
    pltpu.make_async_remote_copy(src_ref=src, dst_ref=dst, send_sem=send, recv_sem=recv, device_id=to, device_id_type=MESH).start()


def await_bytes(ref, sem):
    pltpu.make_async_copy(ref, ref, sem).wait()


def spots(kind, p):
    if kind == TALL:
        return [((p % 3, FULL, pl.ds(p // 3 * TILES * HEAD, TILES * HEAD)), ())]
    if kind == WIDE:
        return [((FULL, FULL, lanes(p)), ())]
    some = [((FULL, FULL, lanes(p)), (pl.ds(0, TILES),))]
    return some + [((p, FULL, lanes(PARTS)), (TILES,))] if p < TILES else some


def cuts(kind, hbm, vmem, core):
    if kind == TALL:
        return [(hbm[0].at[:, :, :, core], vmem)]
    pairs = []
    for z in range(RING):
        for i, one in enumerate(hbm):
            at, size = (0, PARTS * HEAD) if i == 0 else (PARTS * HEAD, HEAD)
            c = pl.ds(pl.multiple_of((core * 2 + z % 2) * size, HEAD), size)
            pairs.append((one.at[:, :, z // 2, :, :, c], vmem.at[:, :, z, :, :, pl.ds(at, size)]))
    return pairs


def some(half, k):
    zeros = (0,) * ((k - 1) // 2)
    return half.at[(*zeros, pl.ds(0, 2))] if k % 2 else half.at[(*zeros, 0)]


def taker(refs):
    refs = list(refs)
    return lambda count: [refs.pop(0) for _ in range(count)]


def count_in(kind):
    return 2 if kind == MORE else 1


def flat_refs(kinds, take):
    return [take(1)[0] if kind != TALL else None for kind in kinds]


class Scatter:
    def __init__(self, kinds, ins, outs, scratch):
        n = len(kinds)
        take, given = taker(scratch), taker(ins)
        self.kinds, self.outs = kinds, outs
        self.ins = [given(count_in(kind)) for kind in kinds]
        self.own, self.beside = take(n), take(n)
        self.got = [take(STAGES) for _ in kinds]
        self.flat, self.cut, self.gathered = (flat_refs(kinds, take) for _ in range(3))
        self.load_sem, self.core_send, self.core_recv, self.send_sem, self.recv_sem, self.fix_send, self.fix_recv = take(7)
        self.xyz, self.core = place()

    def start(self):
        core = self.core
        for j, kind in enumerate(self.kinds):
            for src, dst in cuts(kind, self.ins[j], self.beside[j], 1 - core):
                remote(src, dst, self.core_send.at[j], self.core_recv.at[j], device(self.xyz, 1 - core))
            for src, dst in cuts(kind, self.ins[j], self.own[j], core):
                pltpu.make_async_copy(src, dst, self.load_sem.at[j]).start()

    def each(self, j, k, p, slot, cs, ct):
        dims, g = order(p), self.got[j]
        c = [self.xyz[d] for d in dims]
        a, m = masks(p)
        way = (k - 1) // 2
        free = [None, cs, ct]
        where = []
        for i in range(3):
            if i > way:
                where.append(free[i])
            elif i < way:
                where.append(c[i])
            elif k % 2:
                where.append(flip(c[i], a) if slot == 0 else flip(flip(c[i], a), m))
            else:
                where.append(flip(c[i], m))
        index = [None] * 3
        for d, one in zip(dims, where):
            index[d] = one
        others = [index[d] for d in range(3) if d != dims[0]]
        terms = []
        for stage in range(1, k):
            i = (stage - 1) // 2
            tail = others if i == 0 else where[i + 1 :]
            lead = [1 if stage == k - 1 and k % 2 == 0 else 0] if stage % 2 else []
            terms.append((g[stage - 1], (p, *lead, *tail)))
        return tuple(index), terms

    def totals(self, j, p, index, terms):
        for inside, among in spots(self.kinds[j], p):
            total = self.own[j][(*index, *inside)].astype(F32) + self.beside[j][(*index, *inside)].astype(F32)
            for ref, where in terms:
                total = total + ref[(*where, *among)].astype(F32)
            yield inside, total

    def stage(self, j, k):
        own, g = self.own[j], self.got[j]
        if k == 1:
            await_bytes(own, self.load_sem.at[j])
            await_bytes(self.beside[j], self.core_recv.at[j])
        else:
            await_bytes(some(own, k - 1), self.recv_sem.at[j, k - 2])
        if k > STAGES:
            self.last(j, k)
            return
        slots = range(1 + k % 2)

        def put(cs, ct):
            for p in range(PARTS):
                for slot in slots:
                    index, terms = self.each(j, k, p, slot, cs, ct)
                    for inside, total in self.totals(j, p, index, terms):
                        own[(*index, *inside)] = total.astype(BF16)

        way = (k - 1) // 2
        if way == 0:
            pl.loop(0, RING**2)(lambda i: put(i // RING, i % RING))
        elif way == 1:
            pl.loop(0, RING)(lambda i: put(None, i))
        else:
            put(None, None)
        for p in range(PARTS):
            to = partner(self.xyz, self.core, order(p)[way], masks(p)[1 - k % 2])
            for slot in slots:
                index, _ = self.each(j, k, p, slot, FULL, FULL)
                lead = ((p, slot) if k % 2 else (p,)) + (FULL,) * (2 - way)
                for inside, among in spots(self.kinds[j], p):
                    dst = g[k - 1].at[(*lead, *among)]
                    remote(own.at[(*index, *inside)], dst, self.send_sem.at[j, k - 1], self.recv_sem.at[j, k - 1], to)

    def last(self, j, k):
        kind, flat, cut, gathered = self.kinds[j], self.flat[j], self.cut[j], self.gathered[j]
        for p in range(PARTS):
            for inside, total in self.totals(j, p, *self.each(j, k, p, 0, None, None)):
                if kind == TALL:
                    self.outs[j][inside] = total.astype(BF16)
                    continue
                first = 0 if inside[0] == FULL else inside[0]
                flat[8 * first : 8 * first + total.size // HEAD, inside[2]] = total.reshape(-1, HEAD)
        if kind == TALL:
            return
        mine = self.xyz[2] % 2 * 2 + self.core
        for q in range(GROUP):
            cut[q, 0:OWN_ROWS, :] = flat[OWN_ROWS * q : OWN_ROWS * (q + 1), :].astype(BF16)
        for q in range(GROUP):
            @pl.when(mine != q)
            def _():
                remote(cut.at[q], gathered.at[mine], self.fix_send.at[j], self.fix_recv.at[j], in_group(self.xyz, q))

            @pl.when(mine == q)
            def _():
                gathered[q] = cut[q]

    def waves(self):
        n = len(self.kinds)
        return [[(j, wave - j + 1) for j in reversed(range(n)) if 1 <= wave - j + 1 <= STAGES + 1] for wave in range(n + STAGES)]

    def run(self, wave):
        for j, k in wave:
            self.stage(j, k)

    def finish(self):
        for j, kind in enumerate(self.kinds):
            await_bytes(self.beside[j], self.core_send.at[j])
            for k in range(STAGES):
                await_bytes(some(self.own[j], k + 1), self.send_sem.at[j, k])
            if kind != TALL:
                three = self.gathered[j].at[pl.ds(0, GROUP - 1)]
                await_bytes(three, self.fix_recv.at[j])
                await_bytes(three, self.fix_send.at[j])
                self.outs[j][...] = self.gathered[j][...]


WIDE_SHAPE = (RING, RING, 2, TILES, 8, 3072)
SMALL_SHAPE = (RING, RING, 2, TILES, 8, 512)
TALL_SHAPE = (RING, RING, RING, 2, 3, 8, 1280)


def width(kind):
    return (PARTS + 1 if kind == MORE else PARTS) * HEAD


def halves(kinds):
    return [pltpu.VMEM((RING, RING, RING) + ((3, 8, 1280) if kind == TALL else (TILES, 8, width(kind))), BF16) for kind in kinds]


def pieces_of(kind, *lead):
    return pltpu.VMEM((PARTS, *lead) + ((8, TILES * HEAD) if kind == TALL else (TILES + (kind == MORE), 8, HEAD)), BF16)


def wide_scratch(kinds, rows, dtype):
    return [pltpu.VMEM((*rows, width(kind)), dtype) for kind in kinds if kind != TALL]


def own_shapes(kinds):
    return [jax.ShapeDtypeStruct((3, 8, 1280) if kind == TALL else (GROUP, PADDED, width(kind)), BF16) for kind in kinds]


def semaphores(n):
    sem = pltpu.SemaphoreType.DMA
    return [sem((n,))] * 3 + [sem((n, STAGES))] * 2 + [sem((n,))] * 2


def scatter_scratch(kinds):
    scratch = halves(kinds) * 2
    for kind in kinds:
        for lead in ((2, RING, RING), (RING, RING), (2, RING), (RING,), (2,), ()):
            scratch.append(pieces_of(kind, *lead))
    scratch += wide_scratch(kinds, (GROUP_ROWS,), F32)
    scratch += wide_scratch(kinds, (GROUP, PADDED), BF16) * 2
    return scratch + semaphores(len(kinds))


def scatter_inputs(kinds, arrays):
    ins = []
    for kind, given in zip(kinds, arrays):
        if kind == TALL:
            ins.append(given.reshape(TALL_SHAPE))
        elif kind == MORE:
            ins += [given[0].reshape(WIDE_SHAPE), given[1].reshape(SMALL_SHAPE)]
        else:
            ins.append(given.reshape(WIDE_SHAPE))
    return ins


def talks(number, mib=63):
    return pltpu.CompilerParams(collective_id=number, has_side_effects=True, vmem_limit_bytes=mib * MIB)


ANYWHERE, ON_CHIP = pl.BlockSpec(memory_space=pl.ANY), pl.BlockSpec(memory_space=pltpu.VMEM)


class Gather:
    def __init__(self, kinds, ins, outs, scratch):
        n = len(kinds)
        take, given = taker(scratch), taker(outs)
        self.kinds, self.ins = kinds, ins
        self.outs = [given(count_in(kind)) for kind in kinds]
        self.full = take(n)
        self.flat, self.came = (flat_refs(kinds, take) for _ in range(2))
        self.store_sem, self.core_send, self.core_recv, self.send_sem, self.recv_sem, self.fix_send, self.fix_recv = take(7)
        self.xyz, self.core = place()

    def start(self):
        mine = self.xyz[2] % 2 * 2 + self.core
        for j, kind in enumerate(self.kinds):
            if kind == TALL:
                continue
            for q in range(GROUP):
                @pl.when(mine != q)
                def _():
                    remote(self.ins[j].at[q], self.came[j].at[mine], self.fix_send.at[j], self.fix_recv.at[j], in_group(self.xyz, q))

                @pl.when(mine == q)
                def _():
                    self.came[j][q] = self.ins[j][q]

    def first(self, j):
        kind, o, flat, came = self.kinds[j], self.full[j], self.flat[j], self.came[j]
        if kind == TALL:
            o[self.xyz] = self.ins[j][...]
            return
        await_bytes(came.at[pl.ds(0, GROUP - 1)], self.fix_recv.at[j])
        for q in range(GROUP):
            flat[OWN_ROWS * q : OWN_ROWS * (q + 1), :] = came[q, 0:OWN_ROWS, :].astype(F32)
        for t in range(TILES):
            o[(*self.xyz, t)] = flat[8 * t : 8 * t + 8, :].astype(BF16)

    def stage(self, j, k):
        o = self.full[j]
        if k == STAGES:
            self.first(j)
        else:
            await_bytes(some(o, k + 1), self.recv_sem.at[j, k])
        if k == 0:
            for dst, src in cuts(self.kinds[j], self.outs[j], o, self.core):
                remote(src, dst, self.core_send.at[j], self.core_recv.at[j], device(self.xyz, 1 - self.core))
                pltpu.make_async_copy(src, dst, self.store_sem.at[j]).start()
            return
        way = (k - 1) // 2
        for p in range(PARTS):
            dims = order(p)
            mine = self.xyz[dims[way]]
            held = (mine, flip(mine, masks(p)[1])) if k % 2 else (mine,)
            to = partner(self.xyz, self.core, dims[way], masks(p)[1 - k % 2])
            for one in held:
                index = [FULL] * 3
                for i in range(way):
                    index[dims[i]] = self.xyz[dims[i]]
                index[dims[way]] = one
                for inside, _ in spots(self.kinds[j], p):
                    view = o.at[(*index, *inside)]
                    remote(view, view, self.send_sem.at[j, k - 1], self.recv_sem.at[j, k - 1], to)

    def waves(self):
        n = len(self.kinds)
        return [[(j, k) for j in range(n)] for k in reversed(range(STAGES + 1))]

    run = Scatter.run

    def finish(self):
        for j, kind in enumerate(self.kinds):
            for k in range(1, STAGES + 1):
                await_bytes(some(self.full[j], k), self.send_sem.at[j, k - 1])
            if kind != TALL:
                await_bytes(self.came[j].at[pl.ds(0, GROUP - 1)], self.fix_send.at[j])
            for sem in (self.core_send, self.core_recv, self.store_sem):
                await_bytes(self.full[j], sem.at[j])


def gather_scratch(kinds):
    scratch = halves(kinds)
    scratch += wide_scratch(kinds, (GROUP_ROWS,), F32)
    scratch += wide_scratch(kinds, (GROUP, PADDED), BF16)
    return scratch + semaphores(len(kinds))


def whole_shapes(kinds):
    shapes = []
    for kind in kinds:
        shapes.append(TALL_SHAPE if kind == TALL else WIDE_SHAPE)
        if kind == MORE:
            shapes.append(SMALL_SHAPE)
    return [jax.ShapeDtypeStruct(shape, BF16) for shape in shapes]


def gather(kinds, arrays, number):
    outs = whole_shapes(kinds)

    def kernel(*refs):
        take = taker(refs)
        new = Gather(kinds, take(len(kinds)), take(len(outs)), take(len(gather_scratch(kinds))))
        enter(*place())
        new.start()
        for wave in new.waves():
            new.run(wave)
        new.finish()

    return pl.pallas_call(
        kernel,
        out_shape=outs,
        in_specs=[ON_CHIP] * len(kinds),
        out_specs=[ANYWHERE] * len(outs),
        scratch_shapes=gather_scratch(kinds),
        compiler_params=talks(number, 20),
        name=f"gather{number}",
    )(*arrays)


def exchange(kinds, arrays, new_kinds, new_arrays, number):
    ins, sums_out, outs = scatter_inputs(kinds, arrays), own_shapes(kinds), whole_shapes(new_kinds)
    scratch, new_scratch = scatter_scratch(kinds), gather_scratch(new_kinds)

    def kernel(*refs):
        take = taker(refs)
        ready, rows = take(len(ins)), take(len(new_kinds))
        sums_refs, whole = take(len(sums_out)), take(len(outs))
        sums = Scatter(kinds, ready, sums_refs, take(len(scratch)))
        new = Gather(new_kinds, rows, whole, take(len(new_scratch)))
        enter(*place())
        sums.start()
        new.start()
        ours, theirs = new.waves(), sums.waves()
        for i in range(max(len(ours), len(theirs))):
            for work, waves in ((new, ours), (sums, theirs)):
                for wave in waves[i : i + 1]:
                    work.run(wave)
        sums.finish()
        new.finish()

    got = pl.pallas_call(
        kernel,
        out_shape=sums_out + outs,
        in_specs=[ANYWHERE] * len(ins) + [ON_CHIP] * len(new_kinds),
        out_specs=[ON_CHIP] * len(sums_out) + [ANYWHERE] * len(outs),
        scratch_shapes=scratch + new_scratch,
        compiler_params=talks(number),
        name=f"exchange{number}",
    )(*ins, *new_arrays)
    return got[: len(sums_out)], got[len(sums_out) :]


def attend_bwd(q, k, v, d_out, out, lse, cos, sin, kinds, arrays, number):
    tokens = q.shape[0]
    kv = k.shape[1] // HEAD
    bq = 128
    steps = tokens // bq
    ins, sums_out = scatter_inputs(kinds, arrays), own_shapes(kinds)
    queries = pl.BlockSpec((bq, SPAN), lambda h, i: (i, h))
    keys = pl.BlockSpec((tokens, HEAD), lambda h, i: (0, h))
    table = pl.BlockSpec((tokens, HEAD), lambda h, i: (0, 0))
    count = len(strips(bq))
    own_scratch = [pltpu.VMEM((count, HEAD, STRIP), F32), pltpu.VMEM((tokens, HEAD), F32), pltpu.VMEM((tokens, HEAD), F32),
                   pltpu.VMEM((HEAD, bq), F32), pltpu.VMEM((SPAN, HEAD), BF16)]

    def kernel(*refs):
        take = taker(refs)
        first = take(8)
        ready = take(len(ins))
        last = take(3)
        sums_refs = take(len(sums_out))
        own = take(len(own_scratch))
        sums = Scatter(kinds, ready, sums_refs, take(len(scatter_scratch(kinds))))
        step = pl.program_id(0) * steps + pl.program_id(1)
        waves = sums.waves()
        at_step = {}
        for i, wave in enumerate(waves):
            at_step.setdefault(min(AT[i], kv * steps - 1), []).append(wave)

        @pl.when(step == 0)
        def _():
            enter(*place())
            sums.start()

        backward(*first, *last, *own)
        for n, some in at_step.items():
            @pl.when(step == n)
            def _():
                for wave in some:
                    sums.run(wave)

        @pl.when(step == kv * steps - 1)
        def _():
            sums.finish()

    return pl.pallas_call(
        kernel,
        grid=(kv, steps),
        in_specs=[queries, keys, keys, queries, queries, pl.BlockSpec((1, SPAN // HEAD, bq), lambda h, i: (h, 0, i)), table, table]
        + [ANYWHERE] * len(ins),
        out_specs=[queries, keys, keys] + [ON_CHIP] * len(sums_out),
        out_shape=[jax.ShapeDtypeStruct(one.shape, BF16) for one in (q, k, v)] + sums_out,
        scratch_shapes=own_scratch + scatter_scratch(kinds),
        compiler_params=talks(number),
        name=f"attend_bwd{number}",
    )(q, k, v, d_out, out, lse, cos, sin, *ins)


AT = (1, 3, 6, 10, 12, 13, 14, 15, 15)


def matmul(a, w):
    return jnp.dot(a, w, preferred_element_type=F32).astype(BF16)


def normed(h):
    wide = h.astype(F32)
    scale = lax.rsqrt(jnp.mean(wide**2, -1, keepdims=True) + 1e-6)
    return (wide * scale).astype(BF16)


def projections(a, wq, wk, wv):
    return matmul(a, wq), matmul(a, wk), matmul(a, wv)


def tail(h, mixed, wo, w_gate, w_up, w_down):
    h = h + matmul(mixed, wo)
    b = normed(h)
    gate = jnp.dot(b, w_gate, preferred_element_type=F32)
    up = jnp.dot(b, w_up, preferred_element_type=F32)
    return h + matmul((jax.nn.silu(gate) * up).astype(BF16), w_down)


def adamw(w, m, v, g):
    m = 0.9 * m + 0.1 * g
    v = 0.95 * v + 0.05 * g * g
    step = m * lax.rsqrt(v + 1e-8) + 0.1 * w
    return (w - 0.02 * step).astype(BF16), m, v


def from_quarters(got):
    return got[:, :OWN_ROWS].reshape(2, 2, OWN_ROWS, -1).transpose(2, 1, 0, 3).reshape(OWN_ROWS, -1)


def to_quarters(block):
    cut = block.reshape(OWN_ROWS, 2, 2, -1).transpose(2, 1, 0, 3).reshape(GROUP, OWN_ROWS, -1)
    return jnp.pad(cut, ((0, 0), (0, PADDED - OWN_ROWS), (0, 0)))


LATE, EARLY = (WIDE, WIDE, TALL), (MORE, TALL)


def solution(mesh):
    def step(x, dy, *arrays):
        weights, m, v = (arrays[i : i + 7] for i in (0, 7, 14))
        w = {name: one[0] for name, one in zip(NAMES, weights, strict=True)}
        first, second = (dict(zip(NAMES, some, strict=True)) for some in (m, v))
        cos, sin = angles(x.shape[1])
        h = x[0]
        (q, k, val), back = jax.vjp(functools.partial(projections, normed(h)), w["wq"], w["wk"], w["wv"])
        mixed, lse, q, k = attend(q, k, val, cos, sin)
        _, tail_back = jax.vjp(functools.partial(tail, h), mixed, w["wo"], w["w_gate"], w["w_up"], w["w_down"])
        by_mixed, g_o, g_gate, g_up, g_down = tail_back(dy[0])
        dq, dk, dv, s_gate, s_up, s_down = attend_bwd(q, k, val, by_mixed, mixed, lse, cos, sin, LATE, [g_gate, g_up, g_down], 1)
        g_q, g_k, g_v = back((dq, dk, dv))
        me = lax.axis_index("dp")
        new = {}

        def update(name, g):
            one = first[name]
            rows = one.shape[1]
            own = lax.dynamic_slice_in_dim(w[name], me * rows, rows, 0).astype(F32)
            new[name] = adamw(own, one[0], second[name][0], g.astype(F32))
            return new[name][0]

        def update_tall(name, g):
            return update(name, g.reshape(-1, g.shape[2])).reshape(g.shape)

        update_wide = lambda name, g: to_quarters(update(name, from_quarters(g)))
        late = [update_wide("w_gate", s_gate), update_wide("w_up", s_up), update_tall("w_down", s_down)]
        grads = [(g_q, jnp.concatenate([g_k, g_v], 1)), g_o]
        (s_q, s_o), (gate, up, down) = exchange(EARLY, grads, LATE, late, 2)
        kv = from_quarters(s_q[:, :, PARTS * HEAD :])
        half = kv.shape[1] // 2
        kv = to_quarters(jnp.concatenate([update("wk", kv[:, :half]), update("wv", kv[:, half:])], 1))
        early = [jnp.concatenate([update_wide("wq", s_q[:, :, : PARTS * HEAD]), kv], 2), update_tall("wo", s_o)]
        q, kv, o = gather(EARLY, early, 3)
        kv = kv.reshape(-1, kv.shape[-1])
        whole = {"wq": q, "wk": kv[:, :half], "wv": kv[:, half:], "wo": o, "w_gate": gate, "w_up": up, "w_down": down}
        moments = [new[name][i][None] for i in (1, 2) for name in NAMES]
        return (*(whole[name].reshape(one.shape) for name, one in zip(NAMES, weights, strict=True)), *moments)

    states, all_of, cut = P(("rep", "dp"), None, None), P(None, None, None), P(None, "dp", None)
    return jax.shard_map(
        step,
        mesh=mesh,
        in_specs=(states, states) + (all_of,) * 7 + (cut,) * 14,
        out_specs=(P("rep", None, None),) * 7 + (P("rep", "dp", None),) * 14,
        check_vma=False,
    )
```

```python
import functools

import jax
import jax.numpy as jnp
from jax import lax
from jax.experimental import pallas as pl
from jax.experimental.pallas import tpu as pltpu
from jax.sharding import PartitionSpec as P

NEG = -1e30
HIDDEN = 2 * NEG
LOG2E = 1.4426950408889634
HEAD = 128
THETA = 10000
SPAN = 12 * HEAD
SCALE = HEAD**-0.5
STRIP = 512
KEYS = 256
NAMES = ("wq", "wk", "wv", "wo", "w_gate", "w_up", "w_down")
MIB = 2**20
F32, BF16 = jnp.float32, jnp.bfloat16


def _dot(a, b, ca, cb):
    return lax.dot_general(a, b, (((ca,), (cb,)), ((), ())), preferred_element_type=F32)


def angles(tokens):
    half = HEAD // 2
    angle = jnp.arange(tokens, dtype=F32)[:, None] * THETA ** (-jnp.arange(half, dtype=F32) / half)
    cos, sin = jnp.cos(angle), jnp.sin(angle)
    return jnp.concatenate([cos, cos], 1), jnp.concatenate([-sin, sin], 1)


def swapped(t):
    return pltpu.roll(t, HEAD // 2, 1)


def turn(t, cos, sin):
    t = t.astype(F32)
    return (t * cos + swapped(t) * sin).astype(BF16)


def turn_back(t, cos, sin):
    t = t.astype(BF16).astype(F32)
    return (t * cos + swapped(t * sin)).astype(BF16)


def lanes(n):
    return slice(n * HEAD, (n + 1) * HEAD)


def strips(bq):
    per = STRIP // bq
    return [range(n, n + per) for n in range(0, SPAN // HEAD, per)]


def stacked(ref, heads):
    return jnp.concatenate([ref[:, lanes(n)] for n in heads], axis=0)


def row(ref, heads):
    return jnp.concatenate([ref[n : n + 1, :] for n in heads], axis=1)


def gaps(bq):
    shape = (KEYS, STRIP)
    return lax.rem(lax.broadcasted_iota(jnp.int32, shape, 1), bq) - lax.broadcasted_iota(jnp.int32, shape, 0)


def forward(q_ref, k_ref, v_ref, cos_ref, sin_ref, out_ref, lse_ref, qt_ref, kt_ref, top_s, mix_s):
    bq = q_ref.shape[0]
    iq = pl.program_id(1)
    e = SCALE * LOG2E

    @pl.when(iq == 0)
    def _():
        kt_ref[...] = turn(k_ref[...], cos_ref[...], sin_ref[...])

    here = pl.ds(pl.multiple_of(iq * bq, bq), bq)
    cos, sin = cos_ref[here, :], sin_ref[here, :]
    for n in range(SPAN // HEAD):
        qt_ref[:, lanes(n)] = turn(q_ref[:, lanes(n)], cos, sin)
    top_s[...] = jnp.full_like(top_s, NEG)
    mix_s[...] = jnp.zeros_like(mix_s)
    ones = jnp.ones((8, KEYS), BF16)
    pieces = strips(bq)

    def block(j, masked):
        keys = pl.ds(pl.multiple_of(j * KEYS, KEYS), KEYS)
        values = jnp.concatenate([v_ref[keys, :].T, ones], axis=0)
        scores = [_dot(kt_ref[keys, :], stacked(qt_ref, heads), 1, 1) for heads in pieces]
        weights, keeps = [], []
        for i, s in enumerate(scores):
            if masked:
                s = jnp.where(gaps(bq) >= j * KEYS - iq * bq, s, HIDDEN)
            old = top_s[i : i + 1, :]
            top = jnp.maximum(old, s.max(axis=0, keepdims=True))
            top_s[i : i + 1, :] = top
            weights.append(jnp.exp2((s - top) * e).astype(BF16))
            keeps.append(jnp.exp2((old - top) * e))
        for i, (p, keep) in enumerate(zip(weights, keeps)):
            mix_s[i] = mix_s[i] * keep + _dot(values, p, 1, 0)

    last = (iq * bq) // KEYS
    lax.fori_loop(0, last, lambda j, _: block(j, False), None)
    block(last, True)
    for i, heads in enumerate(pieces):
        total = mix_s[i, HEAD : HEAD + 1, :]
        out = (mix_s[i, :HEAD, :] * (1 / total)).T.astype(BF16)
        lse = top_s[i : i + 1, :] * SCALE + jnp.log(total)
        for at, n in enumerate(heads):
            out_ref[:, lanes(n)] = out[at * bq : (at + 1) * bq, :]
            lse_ref[0, n : n + 1, :] = lse[:, at * bq : (at + 1) * bq]


def attend(q, k, v, cos, sin):
    tokens = q.shape[0]
    kv = k.shape[1] // HEAD
    bq = 256
    queries = pl.BlockSpec((bq, SPAN), lambda h, i: (i, h))
    keys = pl.BlockSpec((tokens, HEAD), lambda h, i: (0, h))
    table = pl.BlockSpec((tokens, HEAD), lambda h, i: (0, 0))
    count = len(strips(bq))
    return pl.pallas_call(
        forward,
        grid=(kv, tokens // bq),
        in_specs=[queries, keys, keys, table, table],
        out_specs=[queries, pl.BlockSpec((1, SPAN // HEAD, bq), lambda h, i: (h, 0, i)), queries, keys],
        out_shape=[jax.ShapeDtypeStruct(q.shape, BF16), jax.ShapeDtypeStruct((kv, SPAN // HEAD, tokens), F32),
                   jax.ShapeDtypeStruct(q.shape, BF16), jax.ShapeDtypeStruct(k.shape, BF16)],
        scratch_shapes=[pltpu.VMEM((count, STRIP), F32), pltpu.VMEM((count, HEAD + 8, STRIP), F32)],
        compiler_params=pltpu.CompilerParams(dimension_semantics=("parallel", "arbitrary"), vmem_limit_bytes=56 * MIB),
        cost_estimate=pl.CostEstimate(flops=4 * q.size * tokens, transcendentals=q.size * tokens // HEAD, bytes_accessed=8 * q.size),
        name="attend",
    )(q, k, v, cos, sin)


def backward(q_ref, k_ref, v_ref, do_ref, out_ref, lse_ref, cos_ref, sin_ref, dq_ref, dk_ref, dv_ref, dq_s, dk_s, dv_s, delta_s, pick_s):
    bq = q_ref.shape[0]
    iq = pl.program_id(1)
    e = SCALE * LOG2E
    pieces = strips(bq)

    @pl.when(iq == 0)
    def _():
        dk_s[...] = jnp.zeros_like(dk_s)
        dv_s[...] = jnp.zeros_like(dv_s)
        of = lax.broadcasted_iota(jnp.int32, pick_s.shape, 0) // HEAD
        pick_s[...] = jnp.where(of == lax.broadcasted_iota(jnp.int32, pick_s.shape, 1), 1.0, 0.0).astype(BF16)

    product = do_ref[...].astype(F32) * out_ref[...].astype(F32)
    high = product.astype(BF16)
    low = (product - high.astype(F32)).astype(BF16)
    delta_s[...] = (_dot(high, pick_s[...], 1, 0) + _dot(low, pick_s[...], 1, 0)).T
    dq_s[...] = jnp.zeros_like(dq_s)

    def block(j, masked):
        keys = pl.ds(pl.multiple_of(j * KEYS, KEYS), KEYS)
        qs = [stacked(q_ref, heads) for heads in pieces]
        dos = [stacked(do_ref, heads) for heads in pieces]
        scores = [_dot(k_ref[keys, :], x, 1, 1) for x in qs]
        dps = [_dot(v_ref[keys, :], x, 1, 1) for x in dos]
        for i, heads in enumerate(pieces):
            p = jnp.exp2(scores[i] * e - row(lse_ref.at[0], heads) * LOG2E)
            if masked:
                p = jnp.where(gaps(bq) >= j * KEYS - iq * bq, p, 0.0)
            ds = (p * (dps[i] - row(delta_s, heads))).astype(BF16)
            dv_s[keys, :] += _dot(p.astype(BF16), dos[i], 1, 0)
            dk_s[keys, :] += _dot(ds, qs[i], 1, 0)
            dq_s[i] += _dot(k_ref[keys, :].T, ds, 1, 0)

    last = (iq * bq) // KEYS
    lax.fori_loop(0, last, lambda j, _: block(j, False), None)
    block(last, True)
    here = pl.ds(pl.multiple_of(iq * bq, bq), bq)
    cos, sin = cos_ref[here, :], sin_ref[here, :]
    for i, heads in enumerate(pieces):
        dq = (dq_s[i] * SCALE).T
        for at, n in enumerate(heads):
            dq_ref[:, lanes(n)] = turn_back(dq[at * bq : (at + 1) * bq, :], cos, sin)

    @pl.when(iq == pl.num_programs(1) - 1)
    def _():
        dk_ref[...] = turn_back(dk_s[...] * SCALE, cos_ref[...], sin_ref[...])
        dv_ref[...] = dv_s[...].astype(BF16)


MESH = pl.DeviceIdType.MESH
RING = 4
PARTS = 6
STAGES = 6
GROUP = 4
GROUP_ROWS = 40
OWN_ROWS = 10
TALL, WIDE, MORE = "tall", "wide", "more"
TILES = 5
PADDED = 16
FULL = slice(None)


def place():
    me = lax.axis_index("dp")
    chip = me // 2
    return (chip // RING**2, chip // RING % RING, chip % RING), me % 2


def flip(c, m):
    return c + 1 - 2 * (c % 2) if m == 1 else RING - 1 - c


def masks(p):
    return (1, RING - 1) if p < PARTS // 2 else (RING - 1, 1)


def order(p):
    return [(p + i) % 3 for i in range(3)]


def device(xyz, core):
    return {"dp": ((xyz[0] * RING + xyz[1]) * RING + xyz[2]) * 2 + core}


def partner(xyz, core, dim, m):
    to = list(xyz)
    to[dim] = flip(to[dim], m)
    return device(to, core)


def in_group(xyz, q):
    return device((*xyz[:2], xyz[2] // 2 * 2 + q // 2), q % 2)


def enter(xyz, core):
    barrier = pltpu.get_barrier_semaphore()
    others = [partner(xyz, core, dim, m) for dim in range(3) for m in masks(0)]
    others += [device(xyz, 1 - core), partner(xyz, 1 - core, 2, 1)]
    for to in others:
        pl.semaphore_signal(barrier, inc=1, device_id=to, device_id_type=MESH)
    pl.semaphore_wait(barrier, len(others))


def remote(src, dst, send, recv, to):
    pltpu.make_async_remote_copy(src_ref=src, dst_ref=dst, send_sem=send, recv_sem=recv, device_id=to, device_id_type=MESH).start()


def await_bytes(ref, sem):
    pltpu.make_async_copy(ref, ref, sem).wait()


def spots(kind, p):
    if kind == TALL:
        return [((p % 3, FULL, pl.ds(p // 3 * TILES * HEAD, TILES * HEAD)), ())]
    if kind == WIDE:
        return [((FULL, FULL, lanes(p)), ())]
    some = [((FULL, FULL, lanes(p)), (pl.ds(0, TILES),))]
    return some + [((p, FULL, lanes(PARTS)), (TILES,))] if p < TILES else some


def cuts(kind, hbm, vmem, core):
    if kind == TALL:
        return [(hbm[0].at[:, :, :, core], vmem)]
    pairs = []
    for z in range(RING):
        for i, one in enumerate(hbm):
            at, size = (0, PARTS * HEAD) if i == 0 else (PARTS * HEAD, HEAD)
            c = pl.ds(pl.multiple_of((core * 2 + z % 2) * size, HEAD), size)
            pairs.append((one.at[:, :, z // 2, :, :, c], vmem.at[:, :, z, :, :, pl.ds(at, size)]))
    return pairs


def some(half, k):
    zeros = (0,) * ((k - 1) // 2)
    return half.at[(*zeros, pl.ds(0, 2))] if k % 2 else half.at[(*zeros, 0)]


def taker(refs):
    refs = list(refs)
    return lambda count: [refs.pop(0) for _ in range(count)]


def count_in(kind):
    return 2 if kind == MORE else 1


def flat_refs(kinds, take):
    return [take(1)[0] if kind != TALL else None for kind in kinds]


class Scatter:
    def __init__(self, kinds, ins, outs, scratch):
        n = len(kinds)
        take, given = taker(scratch), taker(ins)
        self.kinds, self.outs = kinds, outs
        self.ins = [given(count_in(kind)) for kind in kinds]
        self.own, self.beside = take(n), take(n)
        self.got = [take(STAGES) for _ in kinds]
        self.flat, self.cut, self.gathered = (flat_refs(kinds, take) for _ in range(3))
        self.load_sem, self.core_send, self.core_recv, self.send_sem, self.recv_sem, self.fix_send, self.fix_recv = take(7)
        self.xyz, self.core = place()

    def start(self):
        core = self.core
        for j, kind in enumerate(self.kinds):
            for src, dst in cuts(kind, self.ins[j], self.beside[j], 1 - core):
                remote(src, dst, self.core_send.at[j], self.core_recv.at[j], device(self.xyz, 1 - core))
            for src, dst in cuts(kind, self.ins[j], self.own[j], core):
                pltpu.make_async_copy(src, dst, self.load_sem.at[j]).start()

    def each(self, j, k, p, slot, cs, ct):
        dims, g = order(p), self.got[j]
        c = [self.xyz[d] for d in dims]
        a, m = masks(p)
        way = (k - 1) // 2
        free = [None, cs, ct]
        where = []
        for i in range(3):
            if i > way:
                where.append(free[i])
            elif i < way:
                where.append(c[i])
            elif k % 2:
                where.append(flip(c[i], a) if slot == 0 else flip(flip(c[i], a), m))
            else:
                where.append(flip(c[i], m))
        index = [None] * 3
        for d, one in zip(dims, where):
            index[d] = one
        others = [index[d] for d in range(3) if d != dims[0]]
        terms = []
        for stage in range(1, k):
            i = (stage - 1) // 2
            tail = others if i == 0 else where[i + 1 :]
            lead = [1 if stage == k - 1 and k % 2 == 0 else 0] if stage % 2 else []
            terms.append((g[stage - 1], (p, *lead, *tail)))
        return tuple(index), terms

    def totals(self, j, p, index, terms):
        for inside, among in spots(self.kinds[j], p):
            total = self.own[j][(*index, *inside)].astype(F32) + self.beside[j][(*index, *inside)].astype(F32)
            for ref, where in terms:
                total = total + ref[(*where, *among)].astype(F32)
            yield inside, total

    def stage(self, j, k):
        own, g = self.own[j], self.got[j]
        if k == 1:
            await_bytes(own, self.load_sem.at[j])
            await_bytes(self.beside[j], self.core_recv.at[j])
        else:
            await_bytes(some(own, k - 1), self.recv_sem.at[j, k - 2])
        if k > STAGES:
            self.last(j, k)
            return
        slots = range(1 + k % 2)

        def put(cs, ct):
            for p in range(PARTS):
                for slot in slots:
                    index, terms = self.each(j, k, p, slot, cs, ct)
                    for inside, total in self.totals(j, p, index, terms):
                        own[(*index, *inside)] = total.astype(BF16)

        way = (k - 1) // 2
        if way == 0:
            pl.loop(0, RING**2)(lambda i: put(i // RING, i % RING))
        elif way == 1:
            pl.loop(0, RING)(lambda i: put(None, i))
        else:
            put(None, None)
        for p in range(PARTS):
            to = partner(self.xyz, self.core, order(p)[way], masks(p)[1 - k % 2])
            for slot in slots:
                index, _ = self.each(j, k, p, slot, FULL, FULL)
                lead = ((p, slot) if k % 2 else (p,)) + (FULL,) * (2 - way)
                for inside, among in spots(self.kinds[j], p):
                    dst = g[k - 1].at[(*lead, *among)]
                    remote(own.at[(*index, *inside)], dst, self.send_sem.at[j, k - 1], self.recv_sem.at[j, k - 1], to)

    def last(self, j, k):
        kind, flat, cut, gathered = self.kinds[j], self.flat[j], self.cut[j], self.gathered[j]
        for p in range(PARTS):
            for inside, total in self.totals(j, p, *self.each(j, k, p, 0, None, None)):
                if kind == TALL:
                    self.outs[j][inside] = total.astype(BF16)
                    continue
                first = 0 if inside[0] == FULL else inside[0]
                flat[8 * first : 8 * first + total.size // HEAD, inside[2]] = total.reshape(-1, HEAD)
        if kind == TALL:
            return
        mine = self.xyz[2] % 2 * 2 + self.core
        for q in range(GROUP):
            cut[q, 0:OWN_ROWS, :] = flat[OWN_ROWS * q : OWN_ROWS * (q + 1), :].astype(BF16)
        for q in range(GROUP):
            @pl.when(mine != q)
            def _():
                remote(cut.at[q], gathered.at[mine], self.fix_send.at[j], self.fix_recv.at[j], in_group(self.xyz, q))

            @pl.when(mine == q)
            def _():
                gathered[q] = cut[q]

    def waves(self):
        n = len(self.kinds)
        return [[(j, wave - j + 1) for j in reversed(range(n)) if 1 <= wave - j + 1 <= STAGES + 1] for wave in range(n + STAGES)]

    def run(self, wave):
        for j, k in wave:
            self.stage(j, k)

    def finish(self):
        for j, kind in enumerate(self.kinds):
            await_bytes(self.beside[j], self.core_send.at[j])
            for k in range(STAGES):
                await_bytes(some(self.own[j], k + 1), self.send_sem.at[j, k])
            if kind != TALL:
                three = self.gathered[j].at[pl.ds(0, GROUP - 1)]
                await_bytes(three, self.fix_recv.at[j])
                await_bytes(three, self.fix_send.at[j])
                self.outs[j][...] = self.gathered[j][...]


WIDE_SHAPE = (RING, RING, 2, TILES, 8, 3072)
SMALL_SHAPE = (RING, RING, 2, TILES, 8, 512)
TALL_SHAPE = (RING, RING, RING, 2, 3, 8, 1280)


def width(kind):
    return (PARTS + 1 if kind == MORE else PARTS) * HEAD


def halves(kinds):
    return [pltpu.VMEM((RING, RING, RING) + ((3, 8, 1280) if kind == TALL else (TILES, 8, width(kind))), BF16) for kind in kinds]


def pieces_of(kind, *lead):
    return pltpu.VMEM((PARTS, *lead) + ((8, TILES * HEAD) if kind == TALL else (TILES + (kind == MORE), 8, HEAD)), BF16)


def wide_scratch(kinds, rows, dtype):
    return [pltpu.VMEM((*rows, width(kind)), dtype) for kind in kinds if kind != TALL]


def own_shapes(kinds):
    return [jax.ShapeDtypeStruct((3, 8, 1280) if kind == TALL else (GROUP, PADDED, width(kind)), BF16) for kind in kinds]


def semaphores(n):
    sem = pltpu.SemaphoreType.DMA
    return [sem((n,))] * 3 + [sem((n, STAGES))] * 2 + [sem((n,))] * 2


def scatter_scratch(kinds):
    scratch = halves(kinds) * 2
    for kind in kinds:
        for lead in ((2, RING, RING), (RING, RING), (2, RING), (RING,), (2,), ()):
            scratch.append(pieces_of(kind, *lead))
    scratch += wide_scratch(kinds, (GROUP_ROWS,), F32)
    scratch += wide_scratch(kinds, (GROUP, PADDED), BF16) * 2
    return scratch + semaphores(len(kinds))


def scatter_inputs(kinds, arrays):
    ins = []
    for kind, given in zip(kinds, arrays):
        if kind == TALL:
            ins.append(given.reshape(TALL_SHAPE))
        elif kind == MORE:
            ins += [given[0].reshape(WIDE_SHAPE), given[1].reshape(SMALL_SHAPE)]
        else:
            ins.append(given.reshape(WIDE_SHAPE))
    return ins


def talks(number, mib=63):
    return pltpu.CompilerParams(collective_id=number, has_side_effects=True, vmem_limit_bytes=mib * MIB)


ANYWHERE, ON_CHIP = pl.BlockSpec(memory_space=pl.ANY), pl.BlockSpec(memory_space=pltpu.VMEM)


class Gather:
    def __init__(self, kinds, ins, outs, scratch):
        n = len(kinds)
        take, given = taker(scratch), taker(outs)
        self.kinds, self.ins = kinds, ins
        self.outs = [given(count_in(kind)) for kind in kinds]
        self.full = take(n)
        self.flat, self.came = (flat_refs(kinds, take) for _ in range(2))
        self.store_sem, self.core_send, self.core_recv, self.send_sem, self.recv_sem, self.fix_send, self.fix_recv = take(7)
        self.xyz, self.core = place()

    def start(self):
        mine = self.xyz[2] % 2 * 2 + self.core
        for j, kind in enumerate(self.kinds):
            if kind == TALL:
                continue
            for q in range(GROUP):
                @pl.when(mine != q)
                def _():
                    remote(self.ins[j].at[q], self.came[j].at[mine], self.fix_send.at[j], self.fix_recv.at[j], in_group(self.xyz, q))

                @pl.when(mine == q)
                def _():
                    self.came[j][q] = self.ins[j][q]

    def first(self, j):
        kind, o, flat, came = self.kinds[j], self.full[j], self.flat[j], self.came[j]
        if kind == TALL:
            o[self.xyz] = self.ins[j][...]
            return
        await_bytes(came.at[pl.ds(0, GROUP - 1)], self.fix_recv.at[j])
        for q in range(GROUP):
            flat[OWN_ROWS * q : OWN_ROWS * (q + 1), :] = came[q, 0:OWN_ROWS, :].astype(F32)
        for t in range(TILES):
            o[(*self.xyz, t)] = flat[8 * t : 8 * t + 8, :].astype(BF16)

    def stage(self, j, k):
        o = self.full[j]
        if k == STAGES:
            self.first(j)
        else:
            await_bytes(some(o, k + 1), self.recv_sem.at[j, k])
        if k == 0:
            for dst, src in cuts(self.kinds[j], self.outs[j], o, self.core):
                remote(src, dst, self.core_send.at[j], self.core_recv.at[j], device(self.xyz, 1 - self.core))
                pltpu.make_async_copy(src, dst, self.store_sem.at[j]).start()
            return
        way = (k - 1) // 2
        for p in range(PARTS):
            dims = order(p)
            mine = self.xyz[dims[way]]
            held = (mine, flip(mine, masks(p)[1])) if k % 2 else (mine,)
            to = partner(self.xyz, self.core, dims[way], masks(p)[1 - k % 2])
            for one in held:
                index = [FULL] * 3
                for i in range(way):
                    index[dims[i]] = self.xyz[dims[i]]
                index[dims[way]] = one
                for inside, _ in spots(self.kinds[j], p):
                    view = o.at[(*index, *inside)]
                    remote(view, view, self.send_sem.at[j, k - 1], self.recv_sem.at[j, k - 1], to)

    def waves(self):
        n = len(self.kinds)
        return [[(j, k) for j in range(n)] for k in reversed(range(STAGES + 1))]

    run = Scatter.run

    def finish(self):
        for j, kind in enumerate(self.kinds):
            for k in range(1, STAGES + 1):
                await_bytes(some(self.full[j], k), self.send_sem.at[j, k - 1])
            if kind != TALL:
                await_bytes(self.came[j].at[pl.ds(0, GROUP - 1)], self.fix_send.at[j])
            for sem in (self.core_send, self.core_recv, self.store_sem):
                await_bytes(self.full[j], sem.at[j])


def gather_scratch(kinds):
    scratch = halves(kinds)
    scratch += wide_scratch(kinds, (GROUP_ROWS,), F32)
    scratch += wide_scratch(kinds, (GROUP, PADDED), BF16)
    return scratch + semaphores(len(kinds))


def whole_shapes(kinds):
    shapes = []
    for kind in kinds:
        shapes.append(TALL_SHAPE if kind == TALL else WIDE_SHAPE)
        if kind == MORE:
            shapes.append(SMALL_SHAPE)
    return [jax.ShapeDtypeStruct(shape, BF16) for shape in shapes]


def gather(kinds, arrays, number):
    outs = whole_shapes(kinds)

    def kernel(*refs):
        take = taker(refs)
        new = Gather(kinds, take(len(kinds)), take(len(outs)), take(len(gather_scratch(kinds))))
        enter(*place())
        new.start()
        for wave in new.waves():
            new.run(wave)
        new.finish()

    return pl.pallas_call(
        kernel,
        out_shape=outs,
        in_specs=[ON_CHIP] * len(kinds),
        out_specs=[ANYWHERE] * len(outs),
        scratch_shapes=gather_scratch(kinds),
        compiler_params=talks(number, 20),
        name=f"gather{number}",
    )(*arrays)


def exchange(kinds, arrays, new_kinds, new_arrays, number):
    ins, sums_out, outs = scatter_inputs(kinds, arrays), own_shapes(kinds), whole_shapes(new_kinds)
    scratch, new_scratch = scatter_scratch(kinds), gather_scratch(new_kinds)

    def kernel(*refs):
        take = taker(refs)
        ready, rows = take(len(ins)), take(len(new_kinds))
        sums_refs, whole = take(len(sums_out)), take(len(outs))
        sums = Scatter(kinds, ready, sums_refs, take(len(scratch)))
        new = Gather(new_kinds, rows, whole, take(len(new_scratch)))
        enter(*place())
        sums.start()
        new.start()
        ours, theirs = new.waves(), sums.waves()
        for i in range(max(len(ours), len(theirs))):
            for work, waves in ((new, ours), (sums, theirs)):
                for wave in waves[i : i + 1]:
                    work.run(wave)
        sums.finish()
        new.finish()

    got = pl.pallas_call(
        kernel,
        out_shape=sums_out + outs,
        in_specs=[ANYWHERE] * len(ins) + [ON_CHIP] * len(new_kinds),
        out_specs=[ON_CHIP] * len(sums_out) + [ANYWHERE] * len(outs),
        scratch_shapes=scratch + new_scratch,
        compiler_params=talks(number),
        name=f"exchange{number}",
    )(*ins, *new_arrays)
    return got[: len(sums_out)], got[len(sums_out) :]


def deliver(arrays):
    n = len(arrays)

    def kernel(*refs):
        take = taker(refs)
        ins, outs, held = take(n), take(n), take(n)
        (loads, stores) = take(2)
        for i in range(n):
            for c in range(RING):
                pltpu.make_async_copy(ins[i].at[c], held[i].at[c], loads.at[i, c]).start()
        for i in range(n):
            for c in range(RING):
                pltpu.make_async_copy(ins[i].at[c], held[i].at[c], loads.at[i, c]).wait()
                pltpu.make_async_copy(held[i].at[c], outs[i].at[c], stores.at[i, c]).start()
        for i in range(n):
            for c in range(RING):
                pltpu.make_async_copy(held[i].at[c], outs[i].at[c], stores.at[i, c]).wait()

    return pl.pallas_call(
        kernel,
        out_shape=[jax.ShapeDtypeStruct(one.shape, BF16) for one in arrays],
        in_specs=[ANYWHERE] * n,
        out_specs=[ANYWHERE] * n,
        scratch_shapes=[pltpu.VMEM(one.shape, BF16) for one in arrays] + [pltpu.SemaphoreType.DMA((n, RING))] * 2,
        compiler_params=pltpu.CompilerParams(vmem_limit_bytes=VMEM_OF_DELIVER * MIB),
        name="deliver",
    )(*arrays)


VMEM_OF_DELIVER = 60


def attend_bwd(q, k, v, d_out, out, lse, cos, sin, kinds, arrays, number):
    tokens = q.shape[0]
    kv = k.shape[1] // HEAD
    bq = 128
    steps = tokens // bq
    ins, sums_out = scatter_inputs(kinds, arrays), own_shapes(kinds)
    queries = pl.BlockSpec((bq, SPAN), lambda h, i: (i, h))
    keys = pl.BlockSpec((tokens, HEAD), lambda h, i: (0, h))
    table = pl.BlockSpec((tokens, HEAD), lambda h, i: (0, 0))
    count = len(strips(bq))
    own_scratch = [pltpu.VMEM((count, HEAD, STRIP), F32), pltpu.VMEM((tokens, HEAD), F32), pltpu.VMEM((tokens, HEAD), F32),
                   pltpu.VMEM((HEAD, bq), F32), pltpu.VMEM((SPAN, HEAD), BF16)]

    def kernel(*refs):
        take = taker(refs)
        first = take(8)
        ready = take(len(ins))
        last = take(3)
        sums_refs = take(len(sums_out))
        own = take(len(own_scratch))
        sums = Scatter(kinds, ready, sums_refs, take(len(scatter_scratch(kinds))))
        step = pl.program_id(0) * steps + pl.program_id(1)
        waves = sums.waves()
        at_step = {}
        for i, wave in enumerate(waves):
            at_step.setdefault(min(AT[i], kv * steps - 1), []).append(wave)

        @pl.when(step == 0)
        def _():
            enter(*place())
            sums.start()

        backward(*first, *last, *own)
        for n, some in at_step.items():
            @pl.when(step == n)
            def _():
                for wave in some:
                    sums.run(wave)

        @pl.when(step == kv * steps - 1)
        def _():
            sums.finish()

    return pl.pallas_call(
        kernel,
        grid=(kv, steps),
        in_specs=[queries, keys, keys, queries, queries, pl.BlockSpec((1, SPAN // HEAD, bq), lambda h, i: (h, 0, i)), table, table]
        + [ANYWHERE] * len(ins),
        out_specs=[queries, keys, keys] + [ON_CHIP] * len(sums_out),
        out_shape=[jax.ShapeDtypeStruct(one.shape, BF16) for one in (q, k, v)] + sums_out,
        scratch_shapes=own_scratch + scatter_scratch(kinds),
        compiler_params=talks(number),
        name=f"attend_bwd{number}",
    )(q, k, v, d_out, out, lse, cos, sin, *ins)


AT = (1, 3, 6, 10, 12, 13, 14, 15, 15)


def matmul(a, w):
    return jnp.dot(a, w, preferred_element_type=F32).astype(BF16)


def normed(h):
    wide = h.astype(F32)
    scale = lax.rsqrt(jnp.mean(wide**2, -1, keepdims=True) + 1e-6)
    return (wide * scale).astype(BF16)


def projections(a, wq, wk, wv):
    return matmul(a, wq), matmul(a, wk), matmul(a, wv)


def tail(h, mixed, wo, w_gate, w_up, w_down):
    h = h + matmul(mixed, wo)
    b = normed(h)
    gate = jnp.dot(b, w_gate, preferred_element_type=F32)
    up = jnp.dot(b, w_up, preferred_element_type=F32)
    return h + matmul((jax.nn.silu(gate) * up).astype(BF16), w_down)


def adamw(w, m, v, g):
    m = 0.9 * m + 0.1 * g
    v = 0.95 * v + 0.05 * g * g
    step = m * lax.rsqrt(v + 1e-8) + 0.1 * w
    return (w - 0.02 * step).astype(BF16), m, v


def from_quarters(got):
    return got[:, :OWN_ROWS].reshape(2, 2, OWN_ROWS, -1).transpose(2, 1, 0, 3).reshape(OWN_ROWS, -1)


def to_quarters(block):
    cut = block.reshape(OWN_ROWS, 2, 2, -1).transpose(2, 1, 0, 3).reshape(GROUP, OWN_ROWS, -1)
    return jnp.pad(cut, ((0, 0), (0, PADDED - OWN_ROWS), (0, 0)))


LATE, EARLY = (WIDE, WIDE, TALL), (MORE, TALL)


def solution(mesh):
    def step(x, dy, *arrays):
        weights, m, v = (arrays[i : i + 7] for i in (0, 7, 14))
        w = {name: one[0] for name, one in zip(NAMES, weights, strict=True)}
        first, second = (dict(zip(NAMES, some, strict=True)) for some in (m, v))
        cos, sin = angles(x.shape[1])
        h = x[0]
        (q, k, val), back = jax.vjp(functools.partial(projections, normed(h)), w["wq"], w["wk"], w["wv"])
        mixed, lse, q, k = attend(q, k, val, cos, sin)
        _, tail_back = jax.vjp(functools.partial(tail, h), mixed, w["wo"], w["w_gate"], w["w_up"], w["w_down"])
        by_mixed, g_o, g_gate, g_up, g_down = tail_back(dy[0])
        dq, dk, dv, s_gate, s_up, s_down = attend_bwd(q, k, val, by_mixed, mixed, lse, cos, sin, LATE, [g_gate, g_up, g_down], 1)
        g_q, g_k, g_v = back((dq, dk, dv))
        me = lax.axis_index("dp")
        new = {}

        def update(name, g):
            one = first[name]
            rows = one.shape[1]
            own = lax.dynamic_slice_in_dim(w[name], me * rows, rows, 0).astype(F32)
            new[name] = adamw(own, one[0], second[name][0], g.astype(F32))
            return new[name][0]

        def update_tall(name, g):
            return update(name, g.reshape(-1, g.shape[2])).reshape(g.shape)

        update_wide = lambda name, g: to_quarters(update(name, from_quarters(g)))
        late = [update_wide("w_gate", s_gate), update_wide("w_up", s_up), update_tall("w_down", s_down)]
        grads = [(g_q, jnp.concatenate([g_k, g_v], 1)), g_o]
        (s_q, s_o), (gate, up, down) = exchange(EARLY, grads, LATE, late, 2)
        gate, up, down = deliver([gate, up, down])
        kv = from_quarters(s_q[:, :, PARTS * HEAD :])
        half = kv.shape[1] // 2
        kv = to_quarters(jnp.concatenate([update("wk", kv[:, :half]), update("wv", kv[:, half:])], 1))
        early = [jnp.concatenate([update_wide("wq", s_q[:, :, : PARTS * HEAD]), kv], 2), update_tall("wo", s_o)]
        q, kv, o = gather(EARLY, early, 3)
        kv = kv.reshape(-1, kv.shape[-1])
        whole = {"wq": q, "wk": kv[:, :half], "wv": kv[:, half:], "wo": o, "w_gate": gate, "w_up": up, "w_down": down}
        moments = [new[name][i][None] for i in (1, 2) for name in NAMES]
        return (*(whole[name].reshape(one.shape) for name, one in zip(NAMES, weights, strict=True)), *moments)

    states, all_of, cut = P(("rep", "dp"), None, None), P(None, None, None), P(None, "dp", None)
    return jax.shard_map(
        step,
        mesh=mesh,
        in_specs=(states, states) + (all_of,) * 7 + (cut,) * 14,
        out_specs=(P("rep", None, None),) * 7 + (P("rep", "dp", None),) * 14,
        check_vma=False,
    )
```
